32 devices in a mesh: dp: 8 (over y, x, core), mp: 4 (over z).
Axes of the slice: x: 2, y: 2, z: 4, core: 2. Of those that a mesh axis runs over, the one named last changes fastest.
Arguments:
- query_new: bfloat16 [32, 4096], P(('dp', 'mp')), parts along dimension 0, may hold values from -140 to 140
- key_new: bfloat16 [32, 1024], P(('dp', 'mp')), parts along dimension 0, may hold values from -5 to 5
- value_new: bfloat16 [32, 1024], P(('dp', 'mp')), parts along dimension 0, may hold values from -5 to 5
- prefix_keys: bfloat16 [4096, 1024], P(('dp', 'mp')), parts along dimension 0, may hold values from -5 to 5
- prefix_values: bfloat16 [4096, 1024], P(('dp', 'mp')), parts along dimension 0, may hold values from -5 to 5
- sample_suffix_keys: bfloat16 [32, 64, 1024], P(('dp', 'mp')), parts along dimension 0, may hold values from -5 to 5
- sample_suffix_values: bfloat16 [32, 64, 1024], P(('dp', 'mp')), parts along dimension 0, may hold values from -5 to 5
- prefix_len: int32 [8], P('dp'), parts along dimension 0, may hold values from 128 to 512
- suffix_len: int32 [32], P(('dp', 'mp')), parts along dimension 0, may hold values from 1 to 64, as said below
- residual: bfloat16 [32, 8192], P(('dp', 'mp')), parts along dimension 0, may hold values from -3 to 3
- out_weight: bfloat16 [4096, 8192], P('mp'), may hold values from -0.1875 to 0.1875
- norm_gain: bfloat16 [8192], replicated, may hold values from 0.5 to 1.5
Outputs:
- hidden: bfloat16 [32, 8192], P(('dp', 'mp')), parts along dimension 0
- normed: bfloat16 [32, 8192], P(('dp', 'mp')), parts along dimension 0
The draws below stay inside these ranges and needn't reach their ends.
There are 8 independent parts, one for each index of `dp`. The reference program is written for one: setup_inputs(seed, part) draws one part's arguments, and reference() takes and returns one part's arrays. A program takes and returns all parts, laid end to end along the dimension named above; an argument that names none is the same for every part. Nothing has to cross between parts.
Inputs may be any that keep to these rules, and one draw needn't show every extreme that they name: `suffix_len`: some sample has exactly 64 cached generated tokens.
All inputs are finite; a program needn't handle non-finite values.
Results may differ from the reference program's by a relative error of at most 0.0085.
Values may be sent and summed in bfloat16 or wider, within the bound.
A program may use at most 64 MiB of HBM per device.

```python
import jax
import jax.numpy as jnp
from jax import lax

D = 8192
HEAD_SIZE = 128
KEY_VALUE_HEADS = 8
HQ = 32
SUFFIX_POSITIONS = 64
SAMPLE_COUNT = 4
PRE = 512


def joint_keys_queries(key):
    base = jax.random.fold_in(key, 7)
    keys = jnp.clip(jax.random.normal(jax.random.fold_in(base, 1), (PRE, KEY_VALUE_HEADS * HEAD_SIZE), jnp.float32), -5.0, 5.0)
    queries = jnp.clip(2.0 * jax.random.normal(jax.random.fold_in(base, 2), (SAMPLE_COUNT, HQ * HEAD_SIZE), jnp.float32), -8.0, 8.0)
    return (keys, queries)


def draw_prefix_keys(key, part):
    keys, queries = joint_keys_queries(key)
    return keys.astype(jnp.bfloat16)


def draw_query_new(key, part):
    keys, queries = joint_keys_queries(key)
    return queries.astype(jnp.bfloat16)


def draw_suffix_len(key, part):
    base = jax.random.fold_in(key, 31)
    lengths = jax.random.randint(jax.random.fold_in(base, 1), (SAMPLE_COUNT,), 1, SUFFIX_POSITIONS + 1, dtype=jnp.int32)
    chosen = jax.random.randint(jax.random.fold_in(base, 2), (), 0, SAMPLE_COUNT, dtype=jnp.int32)
    lengths = jnp.where(jnp.arange(SAMPLE_COUNT, dtype=jnp.int32) == chosen, SUFFIX_POSITIONS, lengths)
    return lengths.astype(jnp.int32)


def block_levels(stream_key, shape, pieces, low, top_value):
    factor_of, own = 1.0, jax.random.fold_in(stream_key, 6)
    for axis_at, blocks in pieces:
        heights = jnp.exp(jax.random.uniform(jax.random.fold_in(own, axis_at), (blocks,), jnp.float32, low / len(pieces), top_value / len(pieces)))
        factor_of = factor_of * jnp.repeat(heights, shape[axis_at] // blocks).reshape([-1 if axis == axis_at else 1 for axis in range(len(shape))])
    return factor_of


def centred(own_key, shape, deviation, limit, split=(), kind=jnp.bfloat16):
    array = jax.random.normal(own_key, shape, jnp.float32) * deviation
    if len(split) > 0:
        array = block_levels(own_key, shape, split, -0.22, 0.18) * array
    return jnp.clip(array, min=-limit, max=limit).astype(kind)


def setup_inputs(seed: int = 0, part: int = 0) -> dict:
    arg_keys = jax.random.split(jax.random.key(seed), 13)
    part_keys = jax.random.split(jax.random.fold_in(arg_keys[12], part), 13)
    return {
        "query_new": draw_query_new(jax.random.fold_in(jax.random.fold_in(arg_keys[12], part), 71), part),
        "key_new": centred(part_keys[1], (SAMPLE_COUNT, KEY_VALUE_HEADS * HEAD_SIZE), 1.0, 5.0, ((0, 4),)),
        "value_new": centred(part_keys[2], (SAMPLE_COUNT, KEY_VALUE_HEADS * HEAD_SIZE), 1.0, 5.0, ((0, 4),)),
        "prefix_keys": draw_prefix_keys(jax.random.fold_in(jax.random.fold_in(arg_keys[12], part), 71), part),
        "prefix_values": centred(part_keys[4], (PRE, KEY_VALUE_HEADS * HEAD_SIZE), 1.0, 5.0, ((0, 4),)),
        "sample_suffix_keys": centred(part_keys[5], (SAMPLE_COUNT, SUFFIX_POSITIONS, KEY_VALUE_HEADS * HEAD_SIZE), 1.0, 5.0, ((0, 4),)),
        "sample_suffix_values": centred(part_keys[6], (SAMPLE_COUNT, SUFFIX_POSITIONS, KEY_VALUE_HEADS * HEAD_SIZE), 1.0, 5.0, ((0, 4),)),
        "prefix_len": jax.random.randint(part_keys[7], (1,), PRE // 4, PRE + 1).astype(jnp.int32),
        "suffix_len": draw_suffix_len(jax.random.fold_in(jax.random.fold_in(arg_keys[12], part), 71), part),
        "residual": centred(part_keys[9], (SAMPLE_COUNT, D), 0.5, 3.0, ((0, 4),)),
        "out_weight": centred(arg_keys[10], (HQ * HEAD_SIZE, D), (HQ * HEAD_SIZE // 4) ** -0.5, 0.1875, ((0, 4),)),
        "norm_gain": jnp.clip(1.0 + 0.1 * jax.random.normal(arg_keys[11], (D,), jnp.float32), 0.5, 1.5).astype(jnp.bfloat16),
    }


def reference(query_new, key_new, value_new, prefix_keys, prefix_values, sample_suffix_keys, sample_suffix_values, prefix_len, suffix_len, residual, out_weight, norm_gain):
    group = HQ // KEY_VALUE_HEADS
    score_scale = HEAD_SIZE ** (-0.5)
    query_vector = query_new.astype(jnp.float32).reshape(SAMPLE_COUNT, KEY_VALUE_HEADS, group, HEAD_SIZE)
    pkeys = prefix_keys.astype(jnp.float32).reshape(PRE, KEY_VALUE_HEADS, HEAD_SIZE)
    prefix_value_rows = prefix_values.astype(jnp.float32).reshape(PRE, KEY_VALUE_HEADS, HEAD_SIZE)
    suffix_key_rows = sample_suffix_keys.astype(jnp.float32).reshape(SAMPLE_COUNT, SUFFIX_POSITIONS, KEY_VALUE_HEADS, HEAD_SIZE)
    suffix_value_rows = sample_suffix_values.astype(jnp.float32).reshape(SAMPLE_COUNT, SUFFIX_POSITIONS, KEY_VALUE_HEADS, HEAD_SIZE)
    fresh_key_rows = key_new.astype(jnp.float32).reshape(SAMPLE_COUNT, KEY_VALUE_HEADS, HEAD_SIZE)
    nvals = value_new.astype(jnp.float32).reshape(SAMPLE_COUNT, KEY_VALUE_HEADS, HEAD_SIZE)
    pvalid = jnp.arange(PRE, dtype=jnp.int32) < prefix_len[0]
    svalid = jnp.arange(SUFFIX_POSITIONS, dtype=jnp.int32)[None, :] < suffix_len[:, None]
    s_pre = jnp.einsum('bkgd,pkd->bkgp', query_vector, pkeys) * score_scale
    suffix_score_rows = jnp.einsum('cqxt,caqt->cqxa', query_vector, suffix_key_rows) * score_scale
    fresh_score_rows = jnp.einsum('exio,exo->exi', query_vector, fresh_key_rows) * score_scale
    s_pre = jnp.where(pvalid[None, None, None, :], s_pre, -jnp.inf)
    suffix_score_rows = jnp.where(svalid[:, None, None, :], suffix_score_rows, -jnp.inf)
    top = jnp.maximum(jnp.maximum(lax.optimization_barrier(jnp.max(s_pre, -1)), lax.optimization_barrier(jnp.max(suffix_score_rows, -1))), fresh_score_rows)
    w_pre = jnp.exp(s_pre - top[..., None])
    suffix_weight_rows = jnp.exp(suffix_score_rows - top[..., None])
    w_new = jnp.exp(fresh_score_rows - top)
    total = lax.optimization_barrier(jnp.sum(w_pre, -1)) + lax.optimization_barrier(jnp.sum(suffix_weight_rows, -1)) + w_new
    prefix_bias_rows = w_pre.astype(jnp.bfloat16).astype(jnp.float32)
    suffix_bias_rows = suffix_weight_rows.astype(jnp.bfloat16).astype(jnp.float32)
    b_new = w_new.astype(jnp.bfloat16).astype(jnp.float32)
    summed_rows = jnp.einsum('wnso,onr->wnsr', prefix_bias_rows, prefix_value_rows) + jnp.einsum('cjax,cxjq->cjaq', suffix_bias_rows, suffix_value_rows)
    summed_rows = summed_rows + b_new[..., None] * nvals[:, :, None, :]
    attn = (summed_rows / total[..., None]).astype(jnp.bfloat16).reshape(SAMPLE_COUNT, HQ * HEAD_SIZE)
    proj = jnp.dot(attn, out_weight, preferred_element_type=jnp.float32)
    stream = residual.astype(jnp.float32) + proj
    hidden = stream.astype(jnp.bfloat16)
    meansq = lax.optimization_barrier(jnp.mean(stream * stream, axis=-1, keepdims=True))
    normed = (stream * jax.lax.rsqrt(meansq + 1e-05) * norm_gain.astype(jnp.float32)[None, :]).astype(jnp.bfloat16)
    return (hidden, normed)
```

```python
import functools

import jax
import jax.numpy as jnp
from jax import lax
from jax.experimental import pallas as pl
from jax.experimental.pallas import tpu as pltpu
from jax.sharding import PartitionSpec as P

HEAD_SIZE = 128
KEY_VALUE_HEADS = 8
HQ = 32
GROUP = HQ // KEY_VALUE_HEADS
LANES = 128
LOW = -(2.0**100)
CHUNKS = 4
NT = (((1,), (1,)), ((), ()))


def head(ref, k):
    return ref[:, k * HEAD_SIZE : (k + 1) * HEAD_SIZE]


def kernel(
    n,
    plen_ref,
    slen_ref,
    q_hbm,
    kn_hbm,
    vn_hbm,
    pk_hbm,
    pv_hbm,
    sk_hbm,
    sv_hbm,
    res_hbm,
    w_hbm,
    gain_hbm,
    hid_ref,
    nrm_ref,
    qbuf,
    kn,
    vn,
    pk,
    pv,
    sk,
    sv,
    res,
    w,
    gain,
    q_rows,
    m0,
    l0,
    o0,
    pbuf,
    rbuf,
    yacc,
    ysend,
    ybuf,
    local_sem,
    w_sem,
    q_send,
    q_recv,
    p_send,
    p_recv,
    y_send,
    y_recv,
):
    me = lax.axis_index("mp")
    pre = pk.shape[0]
    suf = sk.shape[0]
    rows = pbuf.shape[0]
    part_rows = rows // n
    heads_dev = HQ // n
    width = w.shape[1]
    cw = width // CHUNKS
    crows = cw // LANES
    frows = width // LANES
    scale = HEAD_SIZE ** (-0.5)

    def peer(d):
        return lax.rem(me + d, n)

    local = [
        pltpu.make_async_copy(src, dst, local_sem.at[i])
        for i, (src, dst) in enumerate(
            (
                (q_hbm, qbuf.at[me]),
                (sk_hbm.at[0], sk),
                (kn_hbm, kn),
                (sv_hbm.at[0], sv),
                (vn_hbm, vn),
                (pk_hbm, pk),
                (pv_hbm, pv),
                (res_hbm, res),
                (gain_hbm, gain),
            )
        )
    ]
    for copy in local:
        copy.start()
    w_copies = [
        pltpu.make_async_copy(
            w_hbm.at[:, pl.ds(c * cw, cw)], w.at[:, pl.ds(c * cw, cw)], w_sem.at[c]
        )
        for c in range(CHUNKS)
    ]
    for copy in w_copies:
        copy.start()

    barrier = pltpu.get_barrier_semaphore()
    for d in range(1, n):
        pl.semaphore_signal(
            barrier, inc=1, device_id={"mp": peer(d)}, device_id_type=pl.DeviceIdType.MESH
        )
    pl.semaphore_wait(barrier, n - 1)

    local[0].wait()
    q_copies = []
    for d in range(1, n):
        copy = pltpu.make_async_remote_copy(
            src_ref=qbuf.at[me],
            dst_ref=qbuf.at[me],
            send_sem=q_send.at[d - 1],
            recv_sem=q_recv.at[d - 1],
            device_id={"mp": peer(d)},
            device_id_type=pl.DeviceIdType.MESH,
        )
        copy.start()
        q_copies.append(copy)

    m0[...] = jnp.full(m0.shape, LOW, jnp.float32)
    l0[...] = jnp.zeros(l0.shape, jnp.float32)
    o0[...] = jnp.zeros(o0.shape, jnp.float32)
    own = qbuf[me].astype(jnp.float32).reshape(HQ, HEAD_SIZE)
    own_bf = own.astype(jnp.bfloat16)
    head_of_row = lax.broadcasted_iota(jnp.int32, (HQ, 1), 0) // GROUP
    local[1].wait()
    local[2].wait()
    s_suf = jnp.zeros((HQ, suf), jnp.float32)
    key_rows = jnp.zeros((HQ, HEAD_SIZE), jnp.float32)
    for k in range(KEY_VALUE_HEADS):
        scores = lax.dot_general(own_bf, head(sk, k), NT, preferred_element_type=jnp.float32)
        s_suf = jnp.where(head_of_row == k, scores, s_suf)
        key_rows = jnp.where(head_of_row == k, head(kn, k).astype(jnp.float32), key_rows)
    s_new = jnp.sum(own * key_rows, axis=1, keepdims=True) * scale
    svalid = lax.broadcasted_iota(jnp.int32, (HQ, suf), 1) < slen_ref[0]
    s_suf = jnp.where(svalid, s_suf * scale, LOW)
    top = jnp.maximum(jnp.max(s_suf, axis=1, keepdims=True), s_new)
    w_suf = jnp.where(svalid, jnp.exp(s_suf - top), 0.0)
    w_new = jnp.exp(s_new - top)
    own_total = jnp.sum(w_suf, axis=1, keepdims=True) + w_new
    w_bf = w_suf.astype(jnp.bfloat16)
    local[3].wait()
    local[4].wait()
    own_sum = jnp.zeros((HQ, HEAD_SIZE), jnp.float32)
    value_rows = jnp.zeros((HQ, HEAD_SIZE), jnp.float32)
    for k in range(KEY_VALUE_HEADS):
        sums = jnp.dot(w_bf, head(sv, k), preferred_element_type=jnp.float32)
        own_sum = jnp.where(head_of_row == k, sums, own_sum)
        value_rows = jnp.where(head_of_row == k, head(vn, k).astype(jnp.float32), value_rows)
    own_sum = own_sum + w_new.astype(jnp.bfloat16).astype(jnp.float32) * value_rows
    own_at = pl.ds(me, HQ, stride=n)
    m0[own_at, :] = jnp.broadcast_to(top, (HQ, LANES))
    l0[own_at, :] = jnp.broadcast_to(own_total, (HQ, LANES))
    o0[own_at, :] = own_sum

    local[5].wait()
    local[6].wait()
    for copy in q_copies:
        copy.wait_recv()
    for s in range(n):
        q_rows[pl.ds(s, HQ, stride=n), :] = qbuf[s].astype(jnp.float32).reshape(HQ, HEAD_SIZE)
    q_bf = q_rows[...].astype(jnp.bfloat16)
    per_kv = rows // KEY_VALUE_HEADS
    s_pre = jnp.concatenate(
        [
            lax.dot_general(
                q_bf[k * per_kv : (k + 1) * per_kv],
                head(pk, k),
                NT,
                preferred_element_type=jnp.float32,
            )
            for k in range(KEY_VALUE_HEADS)
        ],
        axis=0,
    )
    pvalid = me * pre + lax.broadcasted_iota(jnp.int32, (rows, pre), 1) < plen_ref[0]
    s_pre = jnp.where(pvalid, s_pre * scale, LOW)
    top0 = m0[...]
    top = jnp.maximum(jnp.max(s_pre, axis=1, keepdims=True), top0)
    top = top.astype(jnp.bfloat16).astype(jnp.float32)
    w_pre = jnp.where(pvalid, jnp.exp(s_pre - top[:, :1]), 0.0)
    keep = jnp.exp(top0 - top)
    total = jnp.sum(w_pre, axis=1, keepdims=True) + l0[...] * keep
    w_bf = w_pre.astype(jnp.bfloat16)
    sums = jnp.concatenate(
        [
            jnp.dot(
                w_bf[k * per_kv : (k + 1) * per_kv],
                head(pv, k),
                preferred_element_type=jnp.float32,
            )
            for k in range(KEY_VALUE_HEADS)
        ],
        axis=0,
    )
    sums = sums + o0[...] * keep
    high = total.astype(jnp.bfloat16).astype(jnp.float32)
    lane = lax.broadcasted_iota(jnp.int32, (rows, LANES), 1)
    stats = jnp.where(lane < 32, top, jnp.where(lane < 64, high, total - high))
    pbuf[:, :LANES] = sums.astype(jnp.bfloat16)
    pbuf[:, LANES:] = stats.astype(jnp.bfloat16)

    p_copies = []
    for d in range(1, n):
        copy = pltpu.make_async_remote_copy(
            src_ref=pbuf.at[pl.ds(pl.multiple_of(peer(d) * part_rows, part_rows), part_rows)],
            dst_ref=rbuf.at[me],
            send_sem=p_send.at[d - 1],
            recv_sem=p_recv.at[d - 1],
            device_id={"mp": peer(d)},
            device_id_type=pl.DeviceIdType.MESH,
        )
        copy.start()
        p_copies.append(copy)
    rbuf[me] = pbuf[pl.ds(pl.multiple_of(me * part_rows, part_rows), part_rows), :]
    for copy in p_copies:
        copy.wait_recv()

    stats = [rbuf[s, :, LANES:].astype(jnp.float32) for s in range(n)]
    tops = [st[:, 0:1] for st in stats]
    best = functools.reduce(jnp.maximum, tops)
    whole_total = jnp.zeros((part_rows, 1), jnp.float32)
    whole_sum = jnp.zeros((part_rows, HEAD_SIZE), jnp.float32)
    for s in range(n):
        factor = jnp.exp(tops[s] - best)
        whole_total = whole_total + factor * (stats[s][:, 32:33] + stats[s][:, 64:65])
        whole_sum = whole_sum + factor * rbuf[s, :, :LANES].astype(jnp.float32)
    attn = whole_sum / whole_total
    attn = jnp.concatenate([attn[h * n : (h + 1) * n] for h in range(heads_dev)], axis=1)
    attn = attn.astype(jnp.bfloat16)

    y_copies = []
    for c in range(CHUNKS):
        w_copies[c].wait()
        y = jnp.dot(attn, w[:, c * cw : (c + 1) * cw], preferred_element_type=jnp.float32)
        for j in range(crows):
            yacc[pl.ds(c * crows + j, n, stride=frows), :] = y[:, j * LANES : (j + 1) * LANES]
        at = pl.ds(c * crows, crows)
        for s in range(n):
            ysend[s, at, :] = yacc[pl.ds(s * frows + c * crows, crows), :].astype(jnp.bfloat16)
        for d in range(1, n):
            copy = pltpu.make_async_remote_copy(
                src_ref=ysend.at[peer(d), at],
                dst_ref=ybuf.at[me, at],
                send_sem=y_send.at[c * (n - 1) + d - 1],
                recv_sem=y_recv.at[c * (n - 1) + d - 1],
                device_id={"mp": peer(d)},
                device_id_type=pl.DeviceIdType.MESH,
            )
            copy.start()
            y_copies.append(copy)

    local[7].wait()
    local[8].wait()
    stream = res[...].astype(jnp.float32).reshape(frows, LANES)
    stream = stream + yacc[pl.ds(pl.multiple_of(me * frows, frows), frows), :]
    for copy in y_copies:
        copy.wait_recv()
    for d in range(1, n):
        stream = stream + ybuf[peer(d)].astype(jnp.float32)
    hid_ref[...] = stream.astype(jnp.bfloat16).reshape(hid_ref.shape)
    meansq = jnp.sum(stream * stream, keepdims=True) / width
    normed = stream * lax.rsqrt(meansq + 1e-05) * gain[...].astype(jnp.float32)
    nrm_ref[...] = normed.astype(jnp.bfloat16).reshape(nrm_ref.shape)
    for copy in q_copies + p_copies + y_copies:
        copy.wait_send()


def local(
    query_new,
    key_new,
    value_new,
    prefix_keys,
    prefix_values,
    sample_suffix_keys,
    sample_suffix_values,
    prefix_len,
    suffix_len,
    residual,
    out_weight,
    norm_gain,
):
    n = lax.axis_size("mp")
    assert query_new.shape[0] == 1
    width = residual.shape[1]
    frows = width // LANES
    rows = HQ * n
    bf, f32 = jnp.bfloat16, jnp.float32
    gain = norm_gain.reshape(frows, LANES)
    smem = pl.BlockSpec(memory_space=pltpu.SMEM)
    hbm = pl.BlockSpec(memory_space=pltpu.HBM)
    vmem = pl.BlockSpec(memory_space=pltpu.VMEM)
    dma = pltpu.SemaphoreType.DMA
    return pl.pallas_call(
        functools.partial(kernel, n),
        out_shape=(
            jax.ShapeDtypeStruct(residual.shape, bf),
            jax.ShapeDtypeStruct(residual.shape, bf),
        ),
        in_specs=[smem, smem] + [hbm] * 10,
        out_specs=(vmem, vmem),
        scratch_shapes=[
            pltpu.VMEM((n,) + query_new.shape, bf),
            pltpu.VMEM(key_new.shape, bf),
            pltpu.VMEM(value_new.shape, bf),
            pltpu.VMEM(prefix_keys.shape, bf),
            pltpu.VMEM(prefix_values.shape, bf),
            pltpu.VMEM(sample_suffix_keys.shape[1:], bf),
            pltpu.VMEM(sample_suffix_values.shape[1:], bf),
            pltpu.VMEM(residual.shape, bf),
            pltpu.VMEM(out_weight.shape, bf),
            pltpu.VMEM(gain.shape, bf),
            pltpu.VMEM((rows, HEAD_SIZE), f32),
            pltpu.VMEM((rows, LANES), f32),
            pltpu.VMEM((rows, LANES), f32),
            pltpu.VMEM((rows, HEAD_SIZE), f32),
            pltpu.VMEM((rows, HEAD_SIZE + LANES), bf),
            pltpu.VMEM((n, rows // n, HEAD_SIZE + LANES), bf),
            pltpu.VMEM((n * frows, LANES), f32),
            pltpu.VMEM((n, frows, LANES), bf),
            pltpu.VMEM((n, frows, LANES), bf),
            dma((9,)),
            dma((CHUNKS,)),
            dma((n - 1,)),
            dma((n - 1,)),
            dma((n - 1,)),
            dma((n - 1,)),
            dma((CHUNKS * (n - 1),)),
            dma((CHUNKS * (n - 1),)),
        ],
        compiler_params=pltpu.CompilerParams(
            collective_id=0, has_side_effects=True, vmem_limit_bytes=40 * 1024 * 1024
        ),
    )(
        prefix_len,
        suffix_len,
        query_new,
        key_new,
        value_new,
        prefix_keys,
        prefix_values,
        sample_suffix_keys,
        sample_suffix_values,
        residual,
        out_weight,
        gain,
    )


def solution(mesh):
    placed = (
        P(("dp", "mp"), None),
        P(("dp", "mp"), None),
        P(("dp", "mp"), None),
        P(("dp", "mp"), None),
        P(("dp", "mp"), None),
        P(("dp", "mp"), None, None),
        P(("dp", "mp"), None, None),
        P("dp"),
        P(("dp", "mp")),
        P(("dp", "mp"), None),
        P("mp", None),
        P(),
    )
    return jax.shard_map(
        local,
        mesh=mesh,
        in_specs=placed,
        out_specs=(P(("dp", "mp"), None), P(("dp", "mp"), None)),
        check_vma=False,
    )
```

```python
import functools

import jax
import jax.numpy as jnp
from jax import lax
from jax.experimental import pallas as pl
from jax.experimental.pallas import tpu as pltpu
from jax.sharding import PartitionSpec as P

HEAD_SIZE = 128
KEY_VALUE_HEADS = 8
HQ = 32
GROUP = HQ // KEY_VALUE_HEADS
LANES = 128
LOW = -(2.0**100)
CHUNKS = 4
NT = (((1,), (1,)), ((), ()))


def head(ref, k):
    return ref[:, k * HEAD_SIZE : (k + 1) * HEAD_SIZE]


def kernel(
    n,
    plen_hbm,
    slen_hbm,
    q_hbm,
    kn_hbm,
    vn_hbm,
    pk_hbm,
    pv_hbm,
    sk_hbm,
    sv_hbm,
    res_hbm,
    w_hbm,
    gain_hbm,
    hid_ref,
    nrm_ref,
    plen_ref,
    slen_ref,
    qbuf,
    kn,
    vn,
    pk,
    pv,
    sk,
    sv,
    res,
    w,
    gain,
    q_rows,
    m0,
    l0,
    o0,
    pbuf,
    rbuf,
    yacc,
    ysend,
    ybuf,
    local_sem,
    w_sem,
    q_send,
    q_recv,
    p_send,
    p_recv,
    y_send,
    y_recv,
):
    me = lax.axis_index("mp")
    pre = pk.shape[0]
    suf = sk.shape[0]
    rows = pbuf.shape[0]
    part_rows = rows // n
    heads_dev = HQ // n
    width = w.shape[1]
    cw = width // CHUNKS
    crows = cw // LANES
    frows = width // LANES
    scale = HEAD_SIZE ** (-0.5)

    def peer(d):
        return lax.rem(me + d, n)

    local = [
        pltpu.make_async_copy(src, dst, local_sem.at[i])
        for i, (src, dst) in enumerate(
            (
                (q_hbm, qbuf.at[me]),
                (sk_hbm.at[0], sk),
                (kn_hbm, kn),
                (sv_hbm.at[0], sv),
                (vn_hbm, vn),
                (pk_hbm, pk),
                (pv_hbm, pv),
                (res_hbm, res),
                (gain_hbm, gain),
                (slen_hbm, slen_ref),
                (plen_hbm, plen_ref),
            )
        )
    ]
    for copy in local:
        copy.start()
    w_copies = [
        pltpu.make_async_copy(
            w_hbm.at[:, pl.ds(c * cw, cw)], w.at[:, pl.ds(c * cw, cw)], w_sem.at[c]
        )
        for c in range(CHUNKS)
    ]
    for copy in w_copies:
        copy.start()

    barrier = pltpu.get_barrier_semaphore()
    for d in range(1, n):
        pl.semaphore_signal(
            barrier, inc=1, device_id={"mp": peer(d)}, device_id_type=pl.DeviceIdType.MESH
        )
    pl.semaphore_wait(barrier, n - 1)

    local[0].wait()
    q_copies = []
    for d in range(1, n):
        copy = pltpu.make_async_remote_copy(
            src_ref=qbuf.at[me],
            dst_ref=qbuf.at[me],
            send_sem=q_send.at[d - 1],
            recv_sem=q_recv.at[d - 1],
            device_id={"mp": peer(d)},
            device_id_type=pl.DeviceIdType.MESH,
        )
        copy.start()
        q_copies.append(copy)

    m0[...] = jnp.full(m0.shape, LOW, jnp.float32)
    l0[...] = jnp.zeros(l0.shape, jnp.float32)
    o0[...] = jnp.zeros(o0.shape, jnp.float32)
    own = qbuf[me].astype(jnp.float32).reshape(HQ, HEAD_SIZE)
    own_bf = own.astype(jnp.bfloat16)
    head_of_row = lax.broadcasted_iota(jnp.int32, (HQ, 1), 0) // GROUP
    local[1].wait()
    local[2].wait()
    s_suf = jnp.zeros((HQ, suf), jnp.float32)
    key_rows = jnp.zeros((HQ, HEAD_SIZE), jnp.float32)
    for k in range(KEY_VALUE_HEADS):
        scores = lax.dot_general(own_bf, head(sk, k), NT, preferred_element_type=jnp.float32)
        s_suf = jnp.where(head_of_row == k, scores, s_suf)
        key_rows = jnp.where(head_of_row == k, head(kn, k).astype(jnp.float32), key_rows)
    s_new = jnp.sum(own * key_rows, axis=1, keepdims=True) * scale
    local[9].wait()
    svalid = lax.broadcasted_iota(jnp.int32, (HQ, suf), 1) < slen_ref[0]
    s_suf = jnp.where(svalid, s_suf * scale, LOW)
    top = jnp.maximum(jnp.max(s_suf, axis=1, keepdims=True), s_new)
    w_suf = jnp.where(svalid, jnp.exp(s_suf - top), 0.0)
    w_new = jnp.exp(s_new - top)
    own_total = jnp.sum(w_suf, axis=1, keepdims=True) + w_new
    w_bf = w_suf.astype(jnp.bfloat16)
    local[3].wait()
    local[4].wait()
    own_sum = jnp.zeros((HQ, HEAD_SIZE), jnp.float32)
    value_rows = jnp.zeros((HQ, HEAD_SIZE), jnp.float32)
    for k in range(KEY_VALUE_HEADS):
        sums = jnp.dot(w_bf, head(sv, k), preferred_element_type=jnp.float32)
        own_sum = jnp.where(head_of_row == k, sums, own_sum)
        value_rows = jnp.where(head_of_row == k, head(vn, k).astype(jnp.float32), value_rows)
    own_sum = own_sum + w_new.astype(jnp.bfloat16).astype(jnp.float32) * value_rows
    own_at = pl.ds(me, HQ, stride=n)
    m0[own_at, :] = jnp.broadcast_to(top, (HQ, LANES))
    l0[own_at, :] = jnp.broadcast_to(own_total, (HQ, LANES))
    o0[own_at, :] = own_sum

    local[5].wait()
    local[6].wait()
    for copy in q_copies:
        copy.wait_recv()
    for s in range(n):
        q_rows[pl.ds(s, HQ, stride=n), :] = qbuf[s].astype(jnp.float32).reshape(HQ, HEAD_SIZE)
    q_bf = q_rows[...].astype(jnp.bfloat16)
    per_kv = rows // KEY_VALUE_HEADS
    s_pre = jnp.concatenate(
        [
            lax.dot_general(
                q_bf[k * per_kv : (k + 1) * per_kv],
                head(pk, k),
                NT,
                preferred_element_type=jnp.float32,
            )
            for k in range(KEY_VALUE_HEADS)
        ],
        axis=0,
    )
    local[10].wait()
    pvalid = me * pre + lax.broadcasted_iota(jnp.int32, (rows, pre), 1) < plen_ref[0]
    s_pre = jnp.where(pvalid, s_pre * scale, LOW)
    top0 = m0[...]
    top = jnp.maximum(jnp.max(s_pre, axis=1, keepdims=True), top0)
    top = top.astype(jnp.bfloat16).astype(jnp.float32)
    w_pre = jnp.where(pvalid, jnp.exp(s_pre - top[:, :1]), 0.0)
    keep = jnp.exp(top0 - top)
    total = jnp.sum(w_pre, axis=1, keepdims=True) + l0[...] * keep
    w_bf = w_pre.astype(jnp.bfloat16)
    sums = jnp.concatenate(
        [
            jnp.dot(
                w_bf[k * per_kv : (k + 1) * per_kv],
                head(pv, k),
                preferred_element_type=jnp.float32,
            )
            for k in range(KEY_VALUE_HEADS)
        ],
        axis=0,
    )
    sums = sums + o0[...] * keep
    high = total.astype(jnp.bfloat16).astype(jnp.float32)
    lane = lax.broadcasted_iota(jnp.int32, (rows, LANES), 1)
    stats = jnp.where(lane < 32, top, jnp.where(lane < 64, high, total - high))
    pbuf[:, :LANES] = sums.astype(jnp.bfloat16)
    pbuf[:, LANES:] = stats.astype(jnp.bfloat16)

    p_copies = []
    for d in range(1, n):
        copy = pltpu.make_async_remote_copy(
            src_ref=pbuf.at[pl.ds(pl.multiple_of(peer(d) * part_rows, part_rows), part_rows)],
            dst_ref=rbuf.at[me],
            send_sem=p_send.at[d - 1],
            recv_sem=p_recv.at[d - 1],
            device_id={"mp": peer(d)},
            device_id_type=pl.DeviceIdType.MESH,
        )
        copy.start()
        p_copies.append(copy)
    rbuf[me] = pbuf[pl.ds(pl.multiple_of(me * part_rows, part_rows), part_rows), :]
    for copy in p_copies:
        copy.wait_recv()

    stats = [rbuf[s, :, LANES:].astype(jnp.float32) for s in range(n)]
    tops = [st[:, 0:1] for st in stats]
    best = functools.reduce(jnp.maximum, tops)
    whole_total = jnp.zeros((part_rows, 1), jnp.float32)
    whole_sum = jnp.zeros((part_rows, HEAD_SIZE), jnp.float32)
    for s in range(n):
        factor = jnp.exp(tops[s] - best)
        whole_total = whole_total + factor * (stats[s][:, 32:33] + stats[s][:, 64:65])
        whole_sum = whole_sum + factor * rbuf[s, :, :LANES].astype(jnp.float32)
    attn = whole_sum / whole_total
    attn = jnp.concatenate([attn[h * n : (h + 1) * n] for h in range(heads_dev)], axis=1)
    attn = attn.astype(jnp.bfloat16)

    y_copies = []
    for c in range(CHUNKS):
        w_copies[c].wait()
        y = jnp.dot(attn, w[:, c * cw : (c + 1) * cw], preferred_element_type=jnp.float32)
        for j in range(crows):
            yacc[pl.ds(c * crows + j, n, stride=frows), :] = y[:, j * LANES : (j + 1) * LANES]
        at = pl.ds(c * crows, crows)
        for s in range(n):
            ysend[s, at, :] = yacc[pl.ds(s * frows + c * crows, crows), :].astype(jnp.bfloat16)
        for d in range(1, n):
            copy = pltpu.make_async_remote_copy(
                src_ref=ysend.at[peer(d), at],
                dst_ref=ybuf.at[me, at],
                send_sem=y_send.at[c * (n - 1) + d - 1],
                recv_sem=y_recv.at[c * (n - 1) + d - 1],
                device_id={"mp": peer(d)},
                device_id_type=pl.DeviceIdType.MESH,
            )
            copy.start()
            y_copies.append(copy)

    local[7].wait()
    local[8].wait()
    stream = res[...].astype(jnp.float32).reshape(frows, LANES)
    stream = stream + yacc[pl.ds(pl.multiple_of(me * frows, frows), frows), :]
    for copy in y_copies:
        copy.wait_recv()
    for d in range(1, n):
        stream = stream + ybuf[peer(d)].astype(jnp.float32)
    hid_ref[...] = stream.astype(jnp.bfloat16).reshape(hid_ref.shape)
    meansq = jnp.sum(stream * stream, keepdims=True) / width
    normed = stream * lax.rsqrt(meansq + 1e-05) * gain[...].astype(jnp.float32)
    nrm_ref[...] = normed.astype(jnp.bfloat16).reshape(nrm_ref.shape)
    for copy in q_copies + p_copies + y_copies:
        copy.wait_send()


def local(
    query_new,
    key_new,
    value_new,
    prefix_keys,
    prefix_values,
    sample_suffix_keys,
    sample_suffix_values,
    prefix_len,
    suffix_len,
    residual,
    out_weight,
    norm_gain,
):
    n = lax.axis_size("mp")
    assert query_new.shape[0] == 1
    width = residual.shape[1]
    frows = width // LANES
    rows = HQ * n
    bf, f32 = jnp.bfloat16, jnp.float32
    gain = norm_gain.reshape(frows, LANES)
    hbm = pl.BlockSpec(memory_space=pltpu.HBM)
    vmem = pl.BlockSpec(memory_space=pltpu.VMEM)
    dma = pltpu.SemaphoreType.DMA
    return pl.pallas_call(
        functools.partial(kernel, n),
        out_shape=(
            jax.ShapeDtypeStruct(residual.shape, bf),
            jax.ShapeDtypeStruct(residual.shape, bf),
        ),
        in_specs=[hbm] * 12,
        out_specs=(vmem, vmem),
        scratch_shapes=[
            pltpu.SMEM(prefix_len.shape, jnp.int32),
            pltpu.SMEM(suffix_len.shape, jnp.int32),
            pltpu.VMEM((n,) + query_new.shape, bf),
            pltpu.VMEM(key_new.shape, bf),
            pltpu.VMEM(value_new.shape, bf),
            pltpu.VMEM(prefix_keys.shape, bf),
            pltpu.VMEM(prefix_values.shape, bf),
            pltpu.VMEM(sample_suffix_keys.shape[1:], bf),
            pltpu.VMEM(sample_suffix_values.shape[1:], bf),
            pltpu.VMEM(residual.shape, bf),
            pltpu.VMEM(out_weight.shape, bf),
            pltpu.VMEM(gain.shape, bf),
            pltpu.VMEM((rows, HEAD_SIZE), f32),
            pltpu.VMEM((rows, LANES), f32),
            pltpu.VMEM((rows, LANES), f32),
            pltpu.VMEM((rows, HEAD_SIZE), f32),
            pltpu.VMEM((rows, HEAD_SIZE + LANES), bf),
            pltpu.VMEM((n, rows // n, HEAD_SIZE + LANES), bf),
            pltpu.VMEM((n * frows, LANES), f32),
            pltpu.VMEM((n, frows, LANES), bf),
            pltpu.VMEM((n, frows, LANES), bf),
            dma((11,)),
            dma((CHUNKS,)),
            dma((n - 1,)),
            dma((n - 1,)),
            dma((n - 1,)),
            dma((n - 1,)),
            dma((CHUNKS * (n - 1),)),
            dma((CHUNKS * (n - 1),)),
        ],
        compiler_params=pltpu.CompilerParams(
            collective_id=0, has_side_effects=True, vmem_limit_bytes=62 * 1024 * 1024
        ),
    )(
        prefix_len,
        suffix_len,
        query_new,
        key_new,
        value_new,
        prefix_keys,
        prefix_values,
        sample_suffix_keys,
        sample_suffix_values,
        residual,
        out_weight,
        gain,
    )


def solution(mesh):
    placed = (
        P(("dp", "mp"), None),
        P(("dp", "mp"), None),
        P(("dp", "mp"), None),
        P(("dp", "mp"), None),
        P(("dp", "mp"), None),
        P(("dp", "mp"), None, None),
        P(("dp", "mp"), None, None),
        P("dp"),
        P(("dp", "mp")),
        P(("dp", "mp"), None),
        P("mp", None),
        P(),
    )
    return jax.shard_map(
        local,
        mesh=mesh,
        in_specs=placed,
        out_specs=(P(("dp", "mp"), None), P(("dp", "mp"), None)),
        check_vma=False,
    )
```

```python
import functools

import jax
import jax.numpy as jnp
from jax import lax
from jax.experimental import pallas as pl
from jax.experimental.pallas import tpu as pltpu
from jax.sharding import PartitionSpec as P

HEAD_SIZE = 128
KEY_VALUE_HEADS = 8
HQ = 32
GROUP = HQ // KEY_VALUE_HEADS
LANES = 128
LOW = -(2.0**100)
CHUNKS = 4
NT = (((1,), (1,)), ((), ()))


def head(ref, k):
    return ref[:, k * HEAD_SIZE : (k + 1) * HEAD_SIZE]


def kernel(
    n,
    plen_hbm,
    slen_hbm,
    q_hbm,
    kn_hbm,
    vn_hbm,
    pk_hbm,
    pv_hbm,
    sk_hbm,
    sv_hbm,
    res_hbm,
    w_hbm,
    gain_hbm,
    hid_ref,
    nrm_ref,
    plen_ref,
    slen_ref,
    qbuf,
    kn,
    vn,
    pk,
    pv,
    sk,
    sv,
    res,
    w,
    gain,
    q_rows,
    m0,
    l0,
    o0,
    pbuf,
    rbuf,
    yacc,
    ysend,
    ybuf,
    local_sem,
    w_sem,
    q_send,
    q_recv,
    p_send,
    p_recv,
    y_send,
    y_recv,
):
    me = lax.axis_index("mp")
    pre = pk.shape[0]
    suf = sk.shape[0]
    rows = pbuf.shape[0]
    part_rows = rows // n
    heads_dev = HQ // n
    width = w.shape[1]
    cw = width // CHUNKS
    crows = cw // LANES
    frows = width // LANES
    scale = HEAD_SIZE ** (-0.5)

    def peer(d):
        return lax.rem(me + d, n)

    local = [
        pltpu.make_async_copy(src, dst, local_sem.at[i])
        for i, (src, dst) in enumerate(
            (
                (q_hbm, qbuf.at[me]),
                (sk_hbm.at[0], sk),
                (kn_hbm, kn),
                (sv_hbm.at[0], sv),
                (vn_hbm, vn),
                (pk_hbm, pk),
                (pv_hbm, pv),
                (res_hbm, res),
                (gain_hbm, gain),
                (slen_hbm, slen_ref),
                (plen_hbm, plen_ref),
            )
        )
    ]
    for copy in local:
        copy.start()
    w_copies = [
        pltpu.make_async_copy(
            w_hbm.at[:, pl.ds(c * cw, cw)], w.at[:, pl.ds(c * cw, cw)], w_sem.at[c]
        )
        for c in range(CHUNKS)
    ]
    for copy in w_copies:
        copy.start()

    barrier = pltpu.get_barrier_semaphore()
    for d in range(1, n):
        pl.semaphore_signal(
            barrier, inc=1, device_id={"mp": peer(d)}, device_id_type=pl.DeviceIdType.MESH
        )
    pl.semaphore_wait(barrier, n - 1)

    local[0].wait()
    q_copies = []
    for d in range(1, n):
        copy = pltpu.make_async_remote_copy(
            src_ref=qbuf.at[me],
            dst_ref=qbuf.at[me],
            send_sem=q_send.at[d - 1],
            recv_sem=q_recv.at[d - 1],
            device_id={"mp": peer(d)},
            device_id_type=pl.DeviceIdType.MESH,
        )
        copy.start()
        q_copies.append(copy)

    m0[...] = jnp.full(m0.shape, LOW, jnp.float32)
    l0[...] = jnp.zeros(l0.shape, jnp.float32)
    o0[...] = jnp.zeros(o0.shape, jnp.float32)
    own = qbuf[me].astype(jnp.float32).reshape(HQ, HEAD_SIZE)
    own_bf = own.astype(jnp.bfloat16)
    head_of_row = lax.broadcasted_iota(jnp.int32, (HQ, 1), 0) // GROUP
    local[1].wait()
    local[2].wait()
    s_suf = jnp.zeros((HQ, suf), jnp.float32)
    key_rows = jnp.zeros((HQ, HEAD_SIZE), jnp.float32)
    for k in range(KEY_VALUE_HEADS):
        scores = lax.dot_general(own_bf, head(sk, k), NT, preferred_element_type=jnp.float32)
        s_suf = jnp.where(head_of_row == k, scores, s_suf)
        key_rows = jnp.where(head_of_row == k, head(kn, k).astype(jnp.float32), key_rows)
    s_new = jnp.sum(own * key_rows, axis=1, keepdims=True) * scale
    local[9].wait()
    svalid = lax.broadcasted_iota(jnp.int32, (HQ, suf), 1) < slen_ref[0]
    s_suf = jnp.where(svalid, s_suf * scale, LOW)
    top = jnp.maximum(jnp.max(s_suf, axis=1, keepdims=True), s_new)
    w_suf = jnp.where(svalid, jnp.exp(s_suf - top), 0.0)
    w_new = jnp.exp(s_new - top)
    own_total = jnp.sum(w_suf, axis=1, keepdims=True) + w_new
    w_bf = w_suf.astype(jnp.bfloat16)
    local[3].wait()
    local[4].wait()
    own_sum = jnp.zeros((HQ, HEAD_SIZE), jnp.float32)
    value_rows = jnp.zeros((HQ, HEAD_SIZE), jnp.float32)
    for k in range(KEY_VALUE_HEADS):
        sums = jnp.dot(w_bf, head(sv, k), preferred_element_type=jnp.float32)
        own_sum = jnp.where(head_of_row == k, sums, own_sum)
        value_rows = jnp.where(head_of_row == k, head(vn, k).astype(jnp.float32), value_rows)
    own_sum = own_sum + w_new.astype(jnp.bfloat16).astype(jnp.float32) * value_rows
    own_at = pl.ds(me, HQ, stride=n)
    m0[own_at, :] = jnp.broadcast_to(top, (HQ, LANES))
    l0[own_at, :] = jnp.broadcast_to(own_total, (HQ, LANES))
    o0[own_at, :] = own_sum

    local[5].wait()
    local[6].wait()
    for copy in q_copies:
        copy.wait_recv()
    for s in range(n):
        q_rows[pl.ds(s, HQ, stride=n), :] = qbuf[s].astype(jnp.float32).reshape(HQ, HEAD_SIZE)
    q_bf = q_rows[...].astype(jnp.bfloat16)
    per_kv = rows // KEY_VALUE_HEADS
    s_pre = jnp.concatenate(
        [
            lax.dot_general(
                q_bf[k * per_kv : (k + 1) * per_kv],
                head(pk, k),
                NT,
                preferred_element_type=jnp.float32,
            )
            for k in range(KEY_VALUE_HEADS)
        ],
        axis=0,
    )
    local[10].wait()
    pvalid = me * pre + lax.broadcasted_iota(jnp.int32, (rows, pre), 1) < plen_ref[0]
    s_pre = jnp.where(pvalid, s_pre * scale, LOW)
    top0 = m0[...]
    top = jnp.maximum(jnp.max(s_pre, axis=1, keepdims=True), top0)
    top = top.astype(jnp.bfloat16).astype(jnp.float32)
    w_pre = jnp.where(pvalid, jnp.exp(s_pre - top[:, :1]), 0.0)
    keep = jnp.exp(top0 - top)
    total = jnp.sum(w_pre, axis=1, keepdims=True) + l0[...] * keep
    w_bf = w_pre.astype(jnp.bfloat16)
    sums = jnp.concatenate(
        [
            jnp.dot(
                w_bf[k * per_kv : (k + 1) * per_kv],
                head(pv, k),
                preferred_element_type=jnp.float32,
            )
            for k in range(KEY_VALUE_HEADS)
        ],
        axis=0,
    )
    sums = sums + o0[...] * keep
    high = total.astype(jnp.bfloat16).astype(jnp.float32)
    lane = lax.broadcasted_iota(jnp.int32, (rows, LANES), 1)
    stats = jnp.where(lane < 32, top, jnp.where(lane < 64, high, total - high))
    pbuf[:, :LANES] = sums.astype(jnp.bfloat16)
    pbuf[:, LANES:] = stats.astype(jnp.bfloat16)

    p_copies = []
    for d in range(1, n):
        copy = pltpu.make_async_remote_copy(
            src_ref=pbuf.at[pl.ds(pl.multiple_of(peer(d) * part_rows, part_rows), part_rows)],
            dst_ref=rbuf.at[me],
            send_sem=p_send.at[d - 1],
            recv_sem=p_recv.at[d - 1],
            device_id={"mp": peer(d)},
            device_id_type=pl.DeviceIdType.MESH,
        )
        copy.start()
        p_copies.append(copy)
    rbuf[me] = pbuf[pl.ds(pl.multiple_of(me * part_rows, part_rows), part_rows), :]
    for copy in p_copies:
        copy.wait_recv()

    stats = [rbuf[s, :, LANES:].astype(jnp.float32) for s in range(n)]
    tops = [st[:, 0:1] for st in stats]
    best = functools.reduce(jnp.maximum, tops)
    whole_total = jnp.zeros((part_rows, 1), jnp.float32)
    whole_sum = jnp.zeros((part_rows, HEAD_SIZE), jnp.float32)
    for s in range(n):
        factor = jnp.exp(tops[s] - best)
        whole_total = whole_total + factor * (stats[s][:, 32:33] + stats[s][:, 64:65])
        whole_sum = whole_sum + factor * rbuf[s, :, :LANES].astype(jnp.float32)
    attn = whole_sum / whole_total
    attn = jnp.concatenate([attn[h * n : (h + 1) * n] for h in range(heads_dev)], axis=1)
    attn = attn.astype(jnp.bfloat16)

    y_copies = []
    for c in range(CHUNKS):
        w_copies[c].wait()
        y = jnp.dot(attn, w[:, c * cw : (c + 1) * cw], preferred_element_type=jnp.float32)
        for j in range(crows):
            yacc[pl.ds(c * crows + j, n, stride=frows), :] = y[:, j * LANES : (j + 1) * LANES]
        at = pl.ds(c * crows, crows)
        for s in range(n):
            ysend[s, at, :] = yacc[pl.ds(s * frows + c * crows, crows), :].astype(jnp.bfloat16)
        for d in range(1, n):
            copy = pltpu.make_async_remote_copy(
                src_ref=ysend.at[peer(d), at],
                dst_ref=ybuf.at[me, at],
                send_sem=y_send.at[c * (n - 1) + d - 1],
                recv_sem=y_recv.at[c * (n - 1) + d - 1],
                device_id={"mp": peer(d)},
                device_id_type=pl.DeviceIdType.MESH,
            )
            copy.start()
            y_copies.append(copy)

    local[7].wait()
    local[8].wait()
    stream = res[...].astype(jnp.float32).reshape(frows, LANES)
    stream = stream + yacc[pl.ds(pl.multiple_of(me * frows, frows), frows), :]
    for copy in y_copies:
        copy.wait_recv()
    for d in range(1, n):
        stream = stream + ybuf[peer(d)].astype(jnp.float32)
    hid_ref[...] = stream.astype(jnp.bfloat16).reshape(hid_ref.shape)
    meansq = jnp.sum(stream * stream, keepdims=True) / width
    normed = stream * lax.rsqrt(meansq + 1e-05) * gain[...].astype(jnp.float32)
    nrm_ref[...] = normed.astype(jnp.bfloat16).reshape(nrm_ref.shape)
    for copy in q_copies + p_copies + y_copies:
        copy.wait_send()


def local(
    query_new,
    key_new,
    value_new,
    prefix_keys,
    prefix_values,
    sample_suffix_keys,
    sample_suffix_values,
    prefix_len,
    suffix_len,
    residual,
    out_weight,
    norm_gain,
):
    n = lax.axis_size("mp")
    assert query_new.shape[0] == 1
    width = residual.shape[1]
    frows = width // LANES
    rows = HQ * n
    bf, f32 = jnp.bfloat16, jnp.float32
    gain = norm_gain.reshape(frows, LANES)
    hbm = pl.BlockSpec(memory_space=pltpu.HBM)
    vmem = pl.BlockSpec(memory_space=pltpu.VMEM)
    dma = pltpu.SemaphoreType.DMA
    return pl.pallas_call(
        functools.partial(kernel, n),
        out_shape=(
            pltpu.VMEM(residual.shape, bf),
            pltpu.VMEM(residual.shape, bf),
        ),
        in_specs=[hbm] * 12,
        out_specs=(vmem, vmem),
        scratch_shapes=[
            pltpu.SMEM(prefix_len.shape, jnp.int32),
            pltpu.SMEM(suffix_len.shape, jnp.int32),
            pltpu.VMEM((n,) + query_new.shape, bf),
            pltpu.VMEM(key_new.shape, bf),
            pltpu.VMEM(value_new.shape, bf),
            pltpu.VMEM(prefix_keys.shape, bf),
            pltpu.VMEM(prefix_values.shape, bf),
            pltpu.VMEM(sample_suffix_keys.shape[1:], bf),
            pltpu.VMEM(sample_suffix_values.shape[1:], bf),
            pltpu.VMEM(residual.shape, bf),
            pltpu.VMEM(out_weight.shape, bf),
            pltpu.VMEM(gain.shape, bf),
            pltpu.VMEM((rows, HEAD_SIZE), f32),
            pltpu.VMEM((rows, LANES), f32),
            pltpu.VMEM((rows, LANES), f32),
            pltpu.VMEM((rows, HEAD_SIZE), f32),
            pltpu.VMEM((rows, HEAD_SIZE + LANES), bf),
            pltpu.VMEM((n, rows // n, HEAD_SIZE + LANES), bf),
            pltpu.VMEM((n * frows, LANES), f32),
            pltpu.VMEM((n, frows, LANES), bf),
            pltpu.VMEM((n, frows, LANES), bf),
            dma((11,)),
            dma((CHUNKS,)),
            dma((n - 1,)),
            dma((n - 1,)),
            dma((n - 1,)),
            dma((n - 1,)),
            dma((CHUNKS * (n - 1),)),
            dma((CHUNKS * (n - 1),)),
        ],
        compiler_params=pltpu.CompilerParams(
            collective_id=0, has_side_effects=True, vmem_limit_bytes=62 * 1024 * 1024
        ),
    )(
        prefix_len,
        suffix_len,
        query_new,
        key_new,
        value_new,
        prefix_keys,
        prefix_values,
        sample_suffix_keys,
        sample_suffix_values,
        residual,
        out_weight,
        gain,
    )


def solution(mesh):
    placed = (
        P(("dp", "mp"), None),
        P(("dp", "mp"), None),
        P(("dp", "mp"), None),
        P(("dp", "mp"), None),
        P(("dp", "mp"), None),
        P(("dp", "mp"), None, None),
        P(("dp", "mp"), None, None),
        P("dp"),
        P(("dp", "mp")),
        P(("dp", "mp"), None),
        P("mp", None),
        P(),
    )
    return jax.shard_map(
        local,
        mesh=mesh,
        in_specs=placed,
        out_specs=(P(("dp", "mp"), None), P(("dp", "mp"), None)),
        check_vma=False,
    )
```

```python
import functools

import jax
import jax.numpy as jnp
from jax import lax
from jax.experimental import pallas as pl
from jax.experimental.pallas import tpu as pltpu
from jax.sharding import PartitionSpec as P

HEAD_SIZE = 128
KEY_VALUE_HEADS = 8
HQ = 32
GROUP = HQ // KEY_VALUE_HEADS
LANES = 128
LOW = -(2.0**100)
CHUNKS = 4
NT = (((1,), (1,)), ((), ()))


def head(ref, k):
    return ref[:, k * HEAD_SIZE : (k + 1) * HEAD_SIZE]


def kernel(
    n,
    plen_hbm,
    slen_hbm,
    q_hbm,
    kn_hbm,
    vn_hbm,
    pk_hbm,
    pv_hbm,
    sk_hbm,
    sv_hbm,
    res_hbm,
    w_hbm,
    gain_hbm,
    hid_ref,
    nrm_ref,
    plen_ref,
    slen_ref,
    qbuf,
    kn,
    vn,
    pk,
    pv,
    sk,
    sv,
    res,
    w,
    gain,
    q_rows,
    m0,
    l0,
    o0,
    pbuf,
    rbuf,
    tbuf,
    trecv,
    yacc,
    ysend,
    ybuf,
    local_sem,
    w_sem,
    q_send,
    q_recv,
    t_send,
    t_recv,
    p_send,
    p_recv,
    y_send,
    y_recv,
):
    me = lax.axis_index("mp")
    pre = pk.shape[0]
    suf = sk.shape[0]
    rows = pbuf.shape[0]
    part_rows = rows // n
    heads_dev = HQ // n
    width = w.shape[1]
    cw = width // CHUNKS
    crows = cw // LANES
    frows = width // LANES
    scale = HEAD_SIZE ** (-0.5)

    def peer(d):
        return lax.rem(me + d, n)

    local = [
        pltpu.make_async_copy(src, dst, local_sem.at[i])
        for i, (src, dst) in enumerate(
            (
                (q_hbm, qbuf.at[me]),
                (sk_hbm.at[0], sk),
                (kn_hbm, kn),
                (sv_hbm.at[0], sv),
                (vn_hbm, vn),
                (pk_hbm, pk),
                (pv_hbm, pv),
                (res_hbm, res),
                (gain_hbm, gain),
                (slen_hbm, slen_ref),
                (plen_hbm, plen_ref),
            )
        )
    ]
    for copy in local:
        copy.start()
    w_copies = [
        pltpu.make_async_copy(
            w_hbm.at[:, pl.ds(c * cw, cw)], w.at[:, pl.ds(c * cw, cw)], w_sem.at[c]
        )
        for c in range(CHUNKS)
    ]
    for copy in w_copies:
        copy.start()

    barrier = pltpu.get_barrier_semaphore()
    for d in range(1, n):
        pl.semaphore_signal(
            barrier, inc=1, device_id={"mp": peer(d)}, device_id_type=pl.DeviceIdType.MESH
        )
    m0[...] = jnp.full(m0.shape, LOW, jnp.float32)
    l0[...] = jnp.zeros(l0.shape, jnp.float32)
    o0[...] = jnp.zeros(o0.shape, jnp.float32)
    local[0].wait()
    own = qbuf[me].astype(jnp.float32).reshape(HQ, HEAD_SIZE)
    own_bf = own.astype(jnp.bfloat16)
    head_of_row = lax.broadcasted_iota(jnp.int32, (HQ, 1), 0) // GROUP
    local[1].wait()
    local[2].wait()
    s_suf = jnp.zeros((HQ, suf), jnp.float32)
    key_rows = jnp.zeros((HQ, HEAD_SIZE), jnp.float32)
    for k in range(KEY_VALUE_HEADS):
        scores = lax.dot_general(own_bf, head(sk, k), NT, preferred_element_type=jnp.float32)
        s_suf = jnp.where(head_of_row == k, scores, s_suf)
        key_rows = jnp.where(head_of_row == k, head(kn, k).astype(jnp.float32), key_rows)
    s_new = jnp.sum(own * key_rows, axis=1, keepdims=True) * scale
    local[9].wait()
    svalid = lax.broadcasted_iota(jnp.int32, (HQ, suf), 1) < slen_ref[0]
    s_suf = jnp.where(svalid, s_suf * scale, LOW)
    top = jnp.maximum(jnp.max(s_suf, axis=1, keepdims=True), s_new)
    w_suf = jnp.where(svalid, jnp.exp(s_suf - top), 0.0)
    w_new = jnp.exp(s_new - top)
    own_total = jnp.sum(w_suf, axis=1, keepdims=True) + w_new
    w_bf = w_suf.astype(jnp.bfloat16)
    local[3].wait()
    local[4].wait()
    own_sum = jnp.zeros((HQ, HEAD_SIZE), jnp.float32)
    value_rows = jnp.zeros((HQ, HEAD_SIZE), jnp.float32)
    for k in range(KEY_VALUE_HEADS):
        sums = jnp.dot(w_bf, head(sv, k), preferred_element_type=jnp.float32)
        own_sum = jnp.where(head_of_row == k, sums, own_sum)
        value_rows = jnp.where(head_of_row == k, head(vn, k).astype(jnp.float32), value_rows)
    own_sum = own_sum + w_new.astype(jnp.bfloat16).astype(jnp.float32) * value_rows
    own_at = pl.ds(me, HQ, stride=n)
    m0[own_at, :] = jnp.broadcast_to(top, (HQ, LANES))
    l0[own_at, :] = jnp.broadcast_to(own_total, (HQ, LANES))
    o0[own_at, :] = own_sum

    pl.semaphore_wait(barrier, n - 1)

    q_copies = []
    for d in range(1, n):
        copy = pltpu.make_async_remote_copy(
            src_ref=qbuf.at[me],
            dst_ref=qbuf.at[me],
            send_sem=q_send.at[d - 1],
            recv_sem=q_recv.at[d - 1],
            device_id={"mp": peer(d)},
            device_id_type=pl.DeviceIdType.MESH,
        )
        copy.start()
        q_copies.append(copy)

    local[5].wait()
    local[6].wait()
    for copy in q_copies:
        copy.wait_recv()
    for s in range(n):
        q_rows[pl.ds(s, HQ, stride=n), :] = qbuf[s].astype(jnp.float32).reshape(HQ, HEAD_SIZE)
    q_bf = q_rows[...].astype(jnp.bfloat16)
    per_kv = rows // KEY_VALUE_HEADS
    s_pre = jnp.concatenate(
        [
            lax.dot_general(
                q_bf[k * per_kv : (k + 1) * per_kv],
                head(pk, k),
                NT,
                preferred_element_type=jnp.float32,
            )
            for k in range(KEY_VALUE_HEADS)
        ],
        axis=0,
    )
    local[10].wait()
    pvalid = me * pre + lax.broadcasted_iota(jnp.int32, (rows, pre), 1) < plen_ref[0]
    s_pre = jnp.where(pvalid, s_pre * scale, LOW)
    top0 = m0[...]
    top = jnp.maximum(jnp.max(s_pre, axis=1, keepdims=True), top0)
    top = top.astype(jnp.bfloat16).astype(jnp.float32)
    w_pre = jnp.where(pvalid, jnp.exp(s_pre - top[:, :1]), 0.0)
    keep = jnp.exp(top0 - top)
    total = jnp.sum(w_pre, axis=1, keepdims=True) + l0[...] * keep
    w_bf = w_pre.astype(jnp.bfloat16)
    diagonal = lax.broadcasted_iota(jnp.int32, (part_rows, LANES), 0) == lax.broadcasted_iota(
        jnp.int32, (part_rows, LANES), 1
    )
    for s in range(n):
        at = slice(s * part_rows, (s + 1) * part_rows)
        for i, column in enumerate((top, total)):
            tbuf[s, i : i + 1, :] = jnp.sum(
                jnp.where(diagonal, column[at], 0.0), axis=0, keepdims=True
            )
    t_copies = []
    for d in range(1, n):
        copy = pltpu.make_async_remote_copy(
            src_ref=tbuf.at[peer(d)],
            dst_ref=trecv.at[me],
            send_sem=t_send.at[d - 1],
            recv_sem=t_recv.at[d - 1],
            device_id={"mp": peer(d)},
            device_id_type=pl.DeviceIdType.MESH,
        )
        t_copies.append(copy)
    sums = jnp.concatenate(
        [
            jnp.dot(
                w_bf[k * per_kv : (k + 1) * per_kv],
                head(pv, k),
                preferred_element_type=jnp.float32,
            )
            for k in range(KEY_VALUE_HEADS)
        ],
        axis=0,
    )
    sums = sums + o0[...] * keep
    pbuf[...] = sums.astype(jnp.bfloat16)
    for copy in t_copies:
        copy.start()

    p_copies = []
    for d in range(1, n):
        copy = pltpu.make_async_remote_copy(
            src_ref=pbuf.at[pl.ds(pl.multiple_of(peer(d) * part_rows, part_rows), part_rows)],
            dst_ref=rbuf.at[me],
            send_sem=p_send.at[d - 1],
            recv_sem=p_recv.at[d - 1],
            device_id={"mp": peer(d)},
            device_id_type=pl.DeviceIdType.MESH,
        )
        copy.start()
        p_copies.append(copy)
    rbuf[me] = pbuf[pl.ds(pl.multiple_of(me * part_rows, part_rows), part_rows), :]
    trecv[me] = tbuf[me]
    for copy in t_copies:
        copy.wait_recv()

    tops = [trecv[s, 0:1, :] for s in range(n)]
    best = functools.reduce(jnp.maximum, tops)
    factors = [jnp.exp(top_s - best) for top_s in tops]
    whole_total = sum(factors[s] * trecv[s, 1:2, :] for s in range(n))
    columns = [
        jnp.sum(jnp.where(diagonal, row, 0.0), axis=1, keepdims=True)
        for row in factors + [whole_total]
    ]
    for copy in p_copies:
        copy.wait_recv()
    whole_sum = sum(columns[s] * rbuf[s].astype(jnp.float32) for s in range(n))
    attn = whole_sum / columns[n]
    attn = jnp.concatenate([attn[h * n : (h + 1) * n] for h in range(heads_dev)], axis=1)
    attn = attn.astype(jnp.bfloat16)

    y_copies = []
    for c in range(CHUNKS):
        w_copies[c].wait()
        y = jnp.dot(attn, w[:, c * cw : (c + 1) * cw], preferred_element_type=jnp.float32)
        for j in range(crows):
            yacc[pl.ds(c * crows + j, n, stride=frows), :] = y[:, j * LANES : (j + 1) * LANES]
        at = pl.ds(c * crows, crows)
        for s in range(n):
            ysend[s, at, :] = yacc[pl.ds(s * frows + c * crows, crows), :].astype(jnp.bfloat16)
        for d in range(1, n):
            copy = pltpu.make_async_remote_copy(
                src_ref=ysend.at[peer(d), at],
                dst_ref=ybuf.at[me, at],
                send_sem=y_send.at[c * (n - 1) + d - 1],
                recv_sem=y_recv.at[c * (n - 1) + d - 1],
                device_id={"mp": peer(d)},
                device_id_type=pl.DeviceIdType.MESH,
            )
            copy.start()
            y_copies.append(copy)

    local[7].wait()
    local[8].wait()
    stream = res[...].astype(jnp.float32).reshape(frows, LANES)
    stream = stream + yacc[pl.ds(pl.multiple_of(me * frows, frows), frows), :]
    for copy in y_copies:
        copy.wait_recv()
    for d in range(1, n):
        stream = stream + ybuf[peer(d)].astype(jnp.float32)
    hid_ref[...] = stream.astype(jnp.bfloat16).reshape(hid_ref.shape)
    meansq = jnp.sum(stream * stream, keepdims=True) / width
    normed = stream * lax.rsqrt(meansq + 1e-05) * gain[...].astype(jnp.float32)
    nrm_ref[...] = normed.astype(jnp.bfloat16).reshape(nrm_ref.shape)
    for copy in q_copies + t_copies + p_copies + y_copies:
        copy.wait_send()


def local(
    query_new,
    key_new,
    value_new,
    prefix_keys,
    prefix_values,
    sample_suffix_keys,
    sample_suffix_values,
    prefix_len,
    suffix_len,
    residual,
    out_weight,
    norm_gain,
):
    n = lax.axis_size("mp")
    assert query_new.shape[0] == 1
    width = residual.shape[1]
    frows = width // LANES
    rows = HQ * n
    bf, f32 = jnp.bfloat16, jnp.float32
    gain = norm_gain.reshape(frows, LANES)
    hbm = pl.BlockSpec(memory_space=pltpu.HBM)
    vmem = pl.BlockSpec(memory_space=pltpu.VMEM)
    dma = pltpu.SemaphoreType.DMA
    return pl.pallas_call(
        functools.partial(kernel, n),
        out_shape=(
            pltpu.VMEM(residual.shape, bf),
            pltpu.VMEM(residual.shape, bf),
        ),
        in_specs=[hbm] * 12,
        out_specs=(vmem, vmem),
        scratch_shapes=[
            pltpu.SMEM(prefix_len.shape, jnp.int32),
            pltpu.SMEM(suffix_len.shape, jnp.int32),
            pltpu.VMEM((n,) + query_new.shape, bf),
            pltpu.VMEM(key_new.shape, bf),
            pltpu.VMEM(value_new.shape, bf),
            pltpu.VMEM(prefix_keys.shape, bf),
            pltpu.VMEM(prefix_values.shape, bf),
            pltpu.VMEM(sample_suffix_keys.shape[1:], bf),
            pltpu.VMEM(sample_suffix_values.shape[1:], bf),
            pltpu.VMEM(residual.shape, bf),
            pltpu.VMEM(out_weight.shape, bf),
            pltpu.VMEM(gain.shape, bf),
            pltpu.VMEM((rows, HEAD_SIZE), f32),
            pltpu.VMEM((rows, LANES), f32),
            pltpu.VMEM((rows, LANES), f32),
            pltpu.VMEM((rows, HEAD_SIZE), f32),
            pltpu.VMEM((rows, HEAD_SIZE), bf),
            pltpu.VMEM((n, rows // n, HEAD_SIZE), bf),
            pltpu.VMEM((n, 2, LANES), f32),
            pltpu.VMEM((n, 2, LANES), f32),
            pltpu.VMEM((n * frows, LANES), f32),
            pltpu.VMEM((n, frows, LANES), bf),
            pltpu.VMEM((n, frows, LANES), bf),
            dma((11,)),
            dma((CHUNKS,)),
            dma((n - 1,)),
            dma((n - 1,)),
            dma((n - 1,)),
            dma((n - 1,)),
            dma((n - 1,)),
            dma((n - 1,)),
            dma((CHUNKS * (n - 1),)),
            dma((CHUNKS * (n - 1),)),
        ],
        compiler_params=pltpu.CompilerParams(
            collective_id=0, has_side_effects=True, vmem_limit_bytes=62 * 1024 * 1024
        ),
    )(
        prefix_len,
        suffix_len,
        query_new,
        key_new,
        value_new,
        prefix_keys,
        prefix_values,
        sample_suffix_keys,
        sample_suffix_values,
        residual,
        out_weight,
        gain,
    )


def solution(mesh):
    placed = (
        P(("dp", "mp"), None),
        P(("dp", "mp"), None),
        P(("dp", "mp"), None),
        P(("dp", "mp"), None),
        P(("dp", "mp"), None),
        P(("dp", "mp"), None, None),
        P(("dp", "mp"), None, None),
        P("dp"),
        P(("dp", "mp")),
        P(("dp", "mp"), None),
        P("mp", None),
        P(),
    )
    return jax.shard_map(
        local,
        mesh=mesh,
        in_specs=placed,
        out_specs=(P(("dp", "mp"), None), P(("dp", "mp"), None)),
        check_vma=False,
    )
```

```python
import functools

import jax
import jax.numpy as jnp
from jax import lax
from jax.experimental import pallas as pl
from jax.experimental.pallas import tpu as pltpu
from jax.sharding import PartitionSpec as P

HEAD_SIZE = 128
KEY_VALUE_HEADS = 8
HQ = 32
GROUP = HQ // KEY_VALUE_HEADS
LANES = 128
LOW = -(2.0**100)
CHUNKS = 4
NT = (((1,), (1,)), ((), ()))


def head(ref, k):
    return ref[:, k * HEAD_SIZE : (k + 1) * HEAD_SIZE]


def kernel(
    n,
    plen_hbm,
    slen_hbm,
    q_hbm,
    kn_hbm,
    vn_hbm,
    pk_hbm,
    pv_hbm,
    sk_hbm,
    sv_hbm,
    res_hbm,
    w_hbm,
    gain_hbm,
    hid_ref,
    nrm_ref,
    plen_ref,
    slen_ref,
    qbuf,
    kn,
    vn,
    pk,
    pv,
    sk,
    sv,
    res,
    w,
    gain,
    q_rows,
    m0,
    l0,
    o0,
    pbuf,
    rbuf,
    tbuf,
    trecv,
    yacc,
    ysend,
    ybuf,
    local_sem,
    w_sem,
    q_send,
    q_recv,
    t_send,
    t_recv,
    p_send,
    p_recv,
    y_send,
    y_recv,
):
    me = lax.axis_index("mp")
    pre = pk.shape[0]
    suf = sk.shape[0]
    rows = pbuf.shape[0]
    part_rows = rows // n
    heads_dev = HQ // n
    width = w.shape[1]
    cw = width // CHUNKS
    crows = cw // LANES
    frows = width // LANES
    scale = HEAD_SIZE ** (-0.5)

    def peer(d):
        return lax.rem(me + d, n)

    local = [
        pltpu.make_async_copy(src, dst, local_sem.at[i])
        for i, (src, dst) in enumerate(
            (
                (q_hbm, qbuf.at[me]),
                (sk_hbm.at[0], sk),
                (kn_hbm, kn),
                (sv_hbm.at[0], sv),
                (vn_hbm, vn),
                (pk_hbm, pk),
                (pv_hbm, pv),
                (res_hbm, res),
                (gain_hbm, gain),
                (slen_hbm, slen_ref),
                (plen_hbm, plen_ref),
            )
        )
    ]
    for copy in local:
        copy.start()
    w_copies = [
        pltpu.make_async_copy(
            w_hbm.at[:, pl.ds(c * cw, cw)], w.at[:, pl.ds(c * cw, cw)], w_sem.at[c]
        )
        for c in range(CHUNKS)
    ]
    for copy in w_copies:
        copy.start()

    barrier = pltpu.get_barrier_semaphore()
    for d in range(1, n):
        pl.semaphore_signal(
            barrier, inc=1, device_id={"mp": peer(d)}, device_id_type=pl.DeviceIdType.MESH
        )
    pl.semaphore_wait(barrier, n - 1)

    local[0].wait()
    q_copies = []
    for d in range(1, n):
        copy = pltpu.make_async_remote_copy(
            src_ref=qbuf.at[me],
            dst_ref=qbuf.at[me],
            send_sem=q_send.at[d - 1],
            recv_sem=q_recv.at[d - 1],
            device_id={"mp": peer(d)},
            device_id_type=pl.DeviceIdType.MESH,
        )
        copy.start()
        q_copies.append(copy)

    m0[...] = jnp.full(m0.shape, LOW, jnp.float32)
    l0[...] = jnp.zeros(l0.shape, jnp.float32)
    o0[...] = jnp.zeros(o0.shape, jnp.float32)
    own = qbuf[me].astype(jnp.float32).reshape(HQ, HEAD_SIZE)
    own_bf = own.astype(jnp.bfloat16)
    head_of_row = lax.broadcasted_iota(jnp.int32, (HQ, 1), 0) // GROUP
    local[1].wait()
    local[2].wait()
    s_suf = jnp.zeros((HQ, suf), jnp.float32)
    key_rows = jnp.zeros((HQ, HEAD_SIZE), jnp.float32)
    for k in range(KEY_VALUE_HEADS):
        scores = lax.dot_general(own_bf, head(sk, k), NT, preferred_element_type=jnp.float32)
        s_suf = jnp.where(head_of_row == k, scores, s_suf)
        key_rows = jnp.where(head_of_row == k, head(kn, k).astype(jnp.float32), key_rows)
    s_new = jnp.sum(own * key_rows, axis=1, keepdims=True) * scale
    local[9].wait()
    svalid = lax.broadcasted_iota(jnp.int32, (HQ, suf), 1) < slen_ref[0]
    s_suf = jnp.where(svalid, s_suf * scale, LOW)
    top = jnp.maximum(jnp.max(s_suf, axis=1, keepdims=True), s_new)
    w_suf = jnp.where(svalid, jnp.exp(s_suf - top), 0.0)
    w_new = jnp.exp(s_new - top)
    own_total = jnp.sum(w_suf, axis=1, keepdims=True) + w_new
    w_bf = w_suf.astype(jnp.bfloat16)
    local[3].wait()
    local[4].wait()
    own_sum = jnp.zeros((HQ, HEAD_SIZE), jnp.float32)
    value_rows = jnp.zeros((HQ, HEAD_SIZE), jnp.float32)
    for k in range(KEY_VALUE_HEADS):
        sums = jnp.dot(w_bf, head(sv, k), preferred_element_type=jnp.float32)
        own_sum = jnp.where(head_of_row == k, sums, own_sum)
        value_rows = jnp.where(head_of_row == k, head(vn, k).astype(jnp.float32), value_rows)
    own_sum = own_sum + w_new.astype(jnp.bfloat16).astype(jnp.float32) * value_rows
    own_at = pl.ds(me, HQ, stride=n)
    m0[own_at, :] = jnp.broadcast_to(top, (HQ, LANES))
    l0[own_at, :] = jnp.broadcast_to(own_total, (HQ, LANES))
    o0[own_at, :] = own_sum

    local[5].wait()
    local[6].wait()
    for copy in q_copies:
        copy.wait_recv()
    for s in range(n):
        q_rows[pl.ds(s, HQ, stride=n), :] = qbuf[s].astype(jnp.float32).reshape(HQ, HEAD_SIZE)
    q_bf = q_rows[...].astype(jnp.bfloat16)
    per_kv = rows // KEY_VALUE_HEADS
    s_pre = jnp.concatenate(
        [
            lax.dot_general(
                q_bf[k * per_kv : (k + 1) * per_kv],
                head(pk, k),
                NT,
                preferred_element_type=jnp.float32,
            )
            for k in range(KEY_VALUE_HEADS)
        ],
        axis=0,
    )
    local[10].wait()
    pvalid = me * pre + lax.broadcasted_iota(jnp.int32, (rows, pre), 1) < plen_ref[0]
    s_pre = jnp.where(pvalid, s_pre * scale, LOW)
    top0 = m0[...]
    top = jnp.maximum(jnp.max(s_pre, axis=1, keepdims=True), top0)
    top = top.astype(jnp.bfloat16).astype(jnp.float32)
    w_pre = jnp.where(pvalid, jnp.exp(s_pre - top[:, :1]), 0.0)
    keep = jnp.exp(top0 - top)
    total = jnp.sum(w_pre, axis=1, keepdims=True) + l0[...] * keep
    w_bf = w_pre.astype(jnp.bfloat16)
    diagonal = lax.broadcasted_iota(jnp.int32, (part_rows, LANES), 0) == lax.broadcasted_iota(
        jnp.int32, (part_rows, LANES), 1
    )
    for s in range(n):
        at = slice(s * part_rows, (s + 1) * part_rows)
        for i, column in enumerate((top, total)):
            tbuf[s, i : i + 1, :] = jnp.sum(
                jnp.where(diagonal, column[at], 0.0), axis=0, keepdims=True
            )
    t_copies = []
    for d in range(1, n):
        copy = pltpu.make_async_remote_copy(
            src_ref=tbuf.at[peer(d)],
            dst_ref=trecv.at[me],
            send_sem=t_send.at[d - 1],
            recv_sem=t_recv.at[d - 1],
            device_id={"mp": peer(d)},
            device_id_type=pl.DeviceIdType.MESH,
        )
        t_copies.append(copy)
    sums = jnp.concatenate(
        [
            jnp.dot(
                w_bf[k * per_kv : (k + 1) * per_kv],
                head(pv, k),
                preferred_element_type=jnp.float32,
            )
            for k in range(KEY_VALUE_HEADS)
        ],
        axis=0,
    )
    sums = sums + o0[...] * keep
    pbuf[...] = sums.astype(jnp.bfloat16)
    for copy in t_copies:
        copy.start()

    p_copies = []
    for d in range(1, n):
        copy = pltpu.make_async_remote_copy(
            src_ref=pbuf.at[pl.ds(pl.multiple_of(peer(d) * part_rows, part_rows), part_rows)],
            dst_ref=rbuf.at[me],
            send_sem=p_send.at[d - 1],
            recv_sem=p_recv.at[d - 1],
            device_id={"mp": peer(d)},
            device_id_type=pl.DeviceIdType.MESH,
        )
        copy.start()
        p_copies.append(copy)
    rbuf[me] = pbuf[pl.ds(pl.multiple_of(me * part_rows, part_rows), part_rows), :]
    trecv[me] = tbuf[me]
    for copy in t_copies:
        copy.wait_recv()

    tops = [trecv[s, 0:1, :] for s in range(n)]
    best = functools.reduce(jnp.maximum, tops)
    factors = [jnp.exp(top_s - best) for top_s in tops]
    whole_total = sum(factors[s] * trecv[s, 1:2, :] for s in range(n))
    columns = [
        jnp.sum(jnp.where(diagonal, row, 0.0), axis=1, keepdims=True)
        for row in factors + [whole_total]
    ]
    for copy in p_copies:
        copy.wait_recv()
    whole_sum = sum(columns[s] * rbuf[s].astype(jnp.float32) for s in range(n))
    attn = whole_sum / columns[n]
    attn = jnp.concatenate([attn[h * n : (h + 1) * n] for h in range(heads_dev)], axis=1)
    attn = attn.astype(jnp.bfloat16)

    y_copies = []
    for c in range(CHUNKS):
        w_copies[c].wait()
        y = jnp.dot(attn, w[:, c * cw : (c + 1) * cw], preferred_element_type=jnp.float32)
        for j in range(crows):
            yacc[pl.ds(c * crows + j, n, stride=frows), :] = y[:, j * LANES : (j + 1) * LANES]
        at = pl.ds(c * crows, crows)
        for s in range(n):
            ysend[s, at, :] = yacc[pl.ds(s * frows + c * crows, crows), :].astype(jnp.bfloat16)
        for d in range(1, n):
            copy = pltpu.make_async_remote_copy(
                src_ref=ysend.at[peer(d), at],
                dst_ref=ybuf.at[me, at],
                send_sem=y_send.at[c * (n - 1) + d - 1],
                recv_sem=y_recv.at[c * (n - 1) + d - 1],
                device_id={"mp": peer(d)},
                device_id_type=pl.DeviceIdType.MESH,
            )
            copy.start()
            y_copies.append(copy)

    local[7].wait()
    local[8].wait()
    stream = res[...].astype(jnp.float32).reshape(frows, LANES)
    stream = stream + yacc[pl.ds(pl.multiple_of(me * frows, frows), frows), :]
    for copy in y_copies:
        copy.wait_recv()
    for d in range(1, n):
        stream = stream + ybuf[peer(d)].astype(jnp.float32)
    hid_ref[...] = stream.astype(jnp.bfloat16).reshape(hid_ref.shape)
    meansq = jnp.sum(stream * stream, keepdims=True) / width
    normed = stream * lax.rsqrt(meansq + 1e-05) * gain[...].astype(jnp.float32)
    nrm_ref[...] = normed.astype(jnp.bfloat16).reshape(nrm_ref.shape)
    for copy in q_copies + t_copies + p_copies + y_copies:
        copy.wait_send()


def local(
    query_new,
    key_new,
    value_new,
    prefix_keys,
    prefix_values,
    sample_suffix_keys,
    sample_suffix_values,
    prefix_len,
    suffix_len,
    residual,
    out_weight,
    norm_gain,
):
    n = lax.axis_size("mp")
    assert query_new.shape[0] == 1
    width = residual.shape[1]
    frows = width // LANES
    rows = HQ * n
    bf, f32 = jnp.bfloat16, jnp.float32
    gain = norm_gain.reshape(frows, LANES)
    hbm = pl.BlockSpec(memory_space=pltpu.HBM)
    vmem = pl.BlockSpec(memory_space=pltpu.VMEM)
    dma = pltpu.SemaphoreType.DMA
    return pl.pallas_call(
        functools.partial(kernel, n),
        out_shape=(
            pltpu.VMEM(residual.shape, bf),
            pltpu.VMEM(residual.shape, bf),
        ),
        in_specs=[hbm] * 12,
        out_specs=(vmem, vmem),
        scratch_shapes=[
            pltpu.SMEM(prefix_len.shape, jnp.int32),
            pltpu.SMEM(suffix_len.shape, jnp.int32),
            pltpu.VMEM((n,) + query_new.shape, bf),
            pltpu.VMEM(key_new.shape, bf),
            pltpu.VMEM(value_new.shape, bf),
            pltpu.VMEM(prefix_keys.shape, bf),
            pltpu.VMEM(prefix_values.shape, bf),
            pltpu.VMEM(sample_suffix_keys.shape[1:], bf),
            pltpu.VMEM(sample_suffix_values.shape[1:], bf),
            pltpu.VMEM(residual.shape, bf),
            pltpu.VMEM(out_weight.shape, bf),
            pltpu.VMEM(gain.shape, bf),
            pltpu.VMEM((rows, HEAD_SIZE), f32),
            pltpu.VMEM((rows, LANES), f32),
            pltpu.VMEM((rows, LANES), f32),
            pltpu.VMEM((rows, HEAD_SIZE), f32),
            pltpu.VMEM((rows, HEAD_SIZE), bf),
            pltpu.VMEM((n, rows // n, HEAD_SIZE), bf),
            pltpu.VMEM((n, 2, LANES), f32),
            pltpu.VMEM((n, 2, LANES), f32),
            pltpu.VMEM((n * frows, LANES), f32),
            pltpu.VMEM((n, frows, LANES), bf),
            pltpu.VMEM((n, frows, LANES), bf),
            dma((11,)),
            dma((CHUNKS,)),
            dma((n - 1,)),
            dma((n - 1,)),
            dma((n - 1,)),
            dma((n - 1,)),
            dma((n - 1,)),
            dma((n - 1,)),
            dma((CHUNKS * (n - 1),)),
            dma((CHUNKS * (n - 1),)),
        ],
        compiler_params=pltpu.CompilerParams(
            collective_id=0, has_side_effects=True, vmem_limit_bytes=62 * 1024 * 1024
        ),
    )(
        prefix_len,
        suffix_len,
        query_new,
        key_new,
        value_new,
        prefix_keys,
        prefix_values,
        sample_suffix_keys,
        sample_suffix_values,
        residual,
        out_weight,
        gain,
    )


def solution(mesh):
    placed = (
        P(("dp", "mp"), None),
        P(("dp", "mp"), None),
        P(("dp", "mp"), None),
        P(("dp", "mp"), None),
        P(("dp", "mp"), None),
        P(("dp", "mp"), None, None),
        P(("dp", "mp"), None, None),
        P("dp"),
        P(("dp", "mp")),
        P(("dp", "mp"), None),
        P("mp", None),
        P(),
    )
    return jax.shard_map(
        local,
        mesh=mesh,
        in_specs=placed,
        out_specs=(P(("dp", "mp"), None), P(("dp", "mp"), None)),
        check_vma=False,
    )
```

```python
import functools

import jax
import jax.numpy as jnp
from jax import lax
from jax.experimental import pallas as pl
from jax.experimental.pallas import tpu as pltpu
from jax.sharding import PartitionSpec as P

HEAD_SIZE = 128
KEY_VALUE_HEADS = 8
HQ = 32
GROUP = HQ // KEY_VALUE_HEADS
LANES = 128
LOW = -(2.0**100)
CHUNKS = 4
NT = (((1,), (1,)), ((), ()))


def head(ref, k):
    return ref[:, k * HEAD_SIZE : (k + 1) * HEAD_SIZE]


def kernel(
    n,
    plen_hbm,
    slen_hbm,
    q_hbm,
    kn_hbm,
    vn_hbm,
    pk_hbm,
    pv_hbm,
    sk_hbm,
    sv_hbm,
    res_hbm,
    w_hbm,
    gain_hbm,
    out_ref,
    plen_ref,
    slen_ref,
    qbuf,
    kn,
    vn,
    pk,
    pv,
    sk,
    sv,
    res,
    w,
    gain,
    q_rows,
    m0,
    l0,
    o0,
    pbuf,
    rbuf,
    tbuf,
    trecv,
    yacc,
    ysend,
    ybuf,
    local_sem,
    w_sem,
    q_send,
    q_recv,
    t_send,
    t_recv,
    p_send,
    p_recv,
    y_send,
    y_recv,
):
    me = lax.axis_index("mp")
    pre = pk.shape[0]
    suf = sk.shape[0]
    rows = pbuf.shape[0]
    part_rows = rows // n
    heads_dev = HQ // n
    width = w.shape[1]
    cw = width // CHUNKS
    crows = cw // LANES
    frows = width // LANES
    scale = HEAD_SIZE ** (-0.5)

    def peer(d):
        return lax.rem(me + d, n)

    local = [
        pltpu.make_async_copy(src, dst, local_sem.at[i])
        for i, (src, dst) in enumerate(
            (
                (q_hbm, qbuf.at[me]),
                (sk_hbm.at[0], sk),
                (kn_hbm, kn),
                (sv_hbm.at[0], sv),
                (vn_hbm, vn),
                (pk_hbm, pk),
                (pv_hbm, pv),
                (res_hbm, res),
                (gain_hbm, gain),
                (slen_hbm, slen_ref),
                (plen_hbm, plen_ref),
            )
        )
    ]
    for copy in local:
        copy.start()
    w_copies = [
        pltpu.make_async_copy(
            w_hbm.at[:, pl.ds(c * cw, cw)], w.at[:, pl.ds(c * cw, cw)], w_sem.at[c]
        )
        for c in range(CHUNKS)
    ]
    for copy in w_copies:
        copy.start()

    barrier = pltpu.get_barrier_semaphore()
    for d in range(1, n):
        pl.semaphore_signal(
            barrier, inc=1, device_id={"mp": peer(d)}, device_id_type=pl.DeviceIdType.MESH
        )
    pl.semaphore_wait(barrier, n - 1)

    local[0].wait()
    q_copies = []
    for d in range(1, n):
        copy = pltpu.make_async_remote_copy(
            src_ref=qbuf.at[me],
            dst_ref=qbuf.at[me],
            send_sem=q_send.at[d - 1],
            recv_sem=q_recv.at[d - 1],
            device_id={"mp": peer(d)},
            device_id_type=pl.DeviceIdType.MESH,
        )
        copy.start()
        q_copies.append(copy)

    m0[...] = jnp.full(m0.shape, LOW, jnp.float32)
    l0[...] = jnp.zeros(l0.shape, jnp.float32)
    o0[...] = jnp.zeros(o0.shape, jnp.float32)
    own = qbuf[me].astype(jnp.float32).reshape(HQ, HEAD_SIZE)
    own_bf = own.astype(jnp.bfloat16)
    head_of_row = lax.broadcasted_iota(jnp.int32, (HQ, 1), 0) // GROUP
    local[1].wait()
    local[2].wait()
    s_suf = jnp.zeros((HQ, suf), jnp.float32)
    key_rows = jnp.zeros((HQ, HEAD_SIZE), jnp.float32)
    for k in range(KEY_VALUE_HEADS):
        scores = lax.dot_general(own_bf, head(sk, k), NT, preferred_element_type=jnp.float32)
        s_suf = jnp.where(head_of_row == k, scores, s_suf)
        key_rows = jnp.where(head_of_row == k, head(kn, k).astype(jnp.float32), key_rows)
    s_new = jnp.sum(own * key_rows, axis=1, keepdims=True) * scale
    local[9].wait()
    svalid = lax.broadcasted_iota(jnp.int32, (HQ, suf), 1) < slen_ref[0]
    s_suf = jnp.where(svalid, s_suf * scale, LOW)
    top = jnp.maximum(jnp.max(s_suf, axis=1, keepdims=True), s_new)
    w_suf = jnp.where(svalid, jnp.exp(s_suf - top), 0.0)
    w_new = jnp.exp(s_new - top)
    own_total = jnp.sum(w_suf, axis=1, keepdims=True) + w_new
    w_bf = w_suf.astype(jnp.bfloat16)
    local[3].wait()
    local[4].wait()
    own_sum = jnp.zeros((HQ, HEAD_SIZE), jnp.float32)
    value_rows = jnp.zeros((HQ, HEAD_SIZE), jnp.float32)
    for k in range(KEY_VALUE_HEADS):
        sums = jnp.dot(w_bf, head(sv, k), preferred_element_type=jnp.float32)
        own_sum = jnp.where(head_of_row == k, sums, own_sum)
        value_rows = jnp.where(head_of_row == k, head(vn, k).astype(jnp.float32), value_rows)
    own_sum = own_sum + w_new.astype(jnp.bfloat16).astype(jnp.float32) * value_rows
    own_at = pl.ds(me, HQ, stride=n)
    m0[own_at, :] = jnp.broadcast_to(top, (HQ, LANES))
    l0[own_at, :] = jnp.broadcast_to(own_total, (HQ, LANES))
    o0[own_at, :] = own_sum

    local[5].wait()
    local[6].wait()
    for copy in q_copies:
        copy.wait_recv()
    for s in range(n):
        q_rows[pl.ds(s, HQ, stride=n), :] = qbuf[s].astype(jnp.float32).reshape(HQ, HEAD_SIZE)
    q_bf = q_rows[...].astype(jnp.bfloat16)
    per_kv = rows // KEY_VALUE_HEADS
    s_pre = jnp.concatenate(
        [
            lax.dot_general(
                q_bf[k * per_kv : (k + 1) * per_kv],
                head(pk, k),
                NT,
                preferred_element_type=jnp.float32,
            )
            for k in range(KEY_VALUE_HEADS)
        ],
        axis=0,
    )
    local[10].wait()
    pvalid = me * pre + lax.broadcasted_iota(jnp.int32, (rows, pre), 1) < plen_ref[0]
    s_pre = jnp.where(pvalid, s_pre * scale, LOW)
    top0 = m0[...]
    top = jnp.maximum(jnp.max(s_pre, axis=1, keepdims=True), top0)
    top = top.astype(jnp.bfloat16).astype(jnp.float32)
    w_pre = jnp.where(pvalid, jnp.exp(s_pre - top[:, :1]), 0.0)
    keep = jnp.exp(top0 - top)
    total = jnp.sum(w_pre, axis=1, keepdims=True) + l0[...] * keep
    w_bf = w_pre.astype(jnp.bfloat16)
    diagonal = lax.broadcasted_iota(jnp.int32, (part_rows, LANES), 0) == lax.broadcasted_iota(
        jnp.int32, (part_rows, LANES), 1
    )
    for s in range(n):
        at = slice(s * part_rows, (s + 1) * part_rows)
        for i, column in enumerate((top, total)):
            tbuf[s, i : i + 1, :] = jnp.sum(
                jnp.where(diagonal, column[at], 0.0), axis=0, keepdims=True
            )
    t_copies = []
    for d in range(1, n):
        copy = pltpu.make_async_remote_copy(
            src_ref=tbuf.at[peer(d)],
            dst_ref=trecv.at[me],
            send_sem=t_send.at[d - 1],
            recv_sem=t_recv.at[d - 1],
            device_id={"mp": peer(d)},
            device_id_type=pl.DeviceIdType.MESH,
        )
        t_copies.append(copy)
    sums = jnp.concatenate(
        [
            jnp.dot(
                w_bf[k * per_kv : (k + 1) * per_kv],
                head(pv, k),
                preferred_element_type=jnp.float32,
            )
            for k in range(KEY_VALUE_HEADS)
        ],
        axis=0,
    )
    sums = sums + o0[...] * keep
    pbuf[...] = sums.astype(jnp.bfloat16)
    for copy in t_copies:
        copy.start()

    p_copies = []
    for d in range(1, n):
        copy = pltpu.make_async_remote_copy(
            src_ref=pbuf.at[pl.ds(pl.multiple_of(peer(d) * part_rows, part_rows), part_rows)],
            dst_ref=rbuf.at[me],
            send_sem=p_send.at[d - 1],
            recv_sem=p_recv.at[d - 1],
            device_id={"mp": peer(d)},
            device_id_type=pl.DeviceIdType.MESH,
        )
        copy.start()
        p_copies.append(copy)
    rbuf[me] = pbuf[pl.ds(pl.multiple_of(me * part_rows, part_rows), part_rows), :]
    trecv[me] = tbuf[me]
    for copy in t_copies:
        copy.wait_recv()

    tops = [trecv[s, 0:1, :] for s in range(n)]
    best = functools.reduce(jnp.maximum, tops)
    factors = [jnp.exp(top_s - best) for top_s in tops]
    whole_total = sum(factors[s] * trecv[s, 1:2, :] for s in range(n))
    columns = [
        jnp.sum(jnp.where(diagonal, row, 0.0), axis=1, keepdims=True)
        for row in factors + [whole_total]
    ]
    for copy in p_copies:
        copy.wait_recv()
    whole_sum = sum(columns[s] * rbuf[s].astype(jnp.float32) for s in range(n))
    attn = whole_sum / columns[n]
    attn = jnp.concatenate([attn[h * n : (h + 1) * n] for h in range(heads_dev)], axis=1)
    attn = attn.astype(jnp.bfloat16)

    y_copies = []
    for c in range(CHUNKS):
        w_copies[c].wait()
        y = jnp.dot(attn, w[:, c * cw : (c + 1) * cw], preferred_element_type=jnp.float32)
        for j in range(crows):
            yacc[pl.ds(c * crows + j, n, stride=frows), :] = y[:, j * LANES : (j + 1) * LANES]
        at = pl.ds(c * crows, crows)
        for s in range(n):
            ysend[s, at, :] = yacc[pl.ds(s * frows + c * crows, crows), :].astype(jnp.bfloat16)
        for d in range(1, n):
            copy = pltpu.make_async_remote_copy(
                src_ref=ysend.at[peer(d), at],
                dst_ref=ybuf.at[me, at],
                send_sem=y_send.at[c * (n - 1) + d - 1],
                recv_sem=y_recv.at[c * (n - 1) + d - 1],
                device_id={"mp": peer(d)},
                device_id_type=pl.DeviceIdType.MESH,
            )
            copy.start()
            y_copies.append(copy)

    local[7].wait()
    local[8].wait()
    stream = res[...].astype(jnp.float32).reshape(frows, LANES)
    stream = stream + yacc[pl.ds(pl.multiple_of(me * frows, frows), frows), :]
    for copy in y_copies:
        copy.wait_recv()
    for d in range(1, n):
        stream = stream + ybuf[peer(d)].astype(jnp.float32)
    out_ref[0:1,:] = stream.astype(jnp.bfloat16).reshape(1,width)
    meansq = jnp.sum(stream * stream, keepdims=True) / width
    normed = stream * lax.rsqrt(meansq + 1e-05) * gain[...].astype(jnp.float32)
    out_ref[1:2,:] = normed.astype(jnp.bfloat16).reshape(1,width)
    for copy in q_copies + t_copies + p_copies + y_copies:
        copy.wait_send()


def local(
    query_new,
    key_new,
    value_new,
    prefix_keys,
    prefix_values,
    sample_suffix_keys,
    sample_suffix_values,
    prefix_len,
    suffix_len,
    residual,
    out_weight,
    norm_gain,
):
    n = lax.axis_size("mp")
    assert query_new.shape[0] == 1
    width = residual.shape[1]
    frows = width // LANES
    rows = HQ * n
    bf, f32 = jnp.bfloat16, jnp.float32
    gain = norm_gain.reshape(frows, LANES)
    hbm = pl.BlockSpec(memory_space=pltpu.HBM)
    vmem = pl.BlockSpec(memory_space=pltpu.VMEM)
    dma = pltpu.SemaphoreType.DMA
    o = pl.pallas_call(
        functools.partial(kernel, n),
        out_shape=pltpu.VMEM((2, width), bf),
        in_specs=[hbm] * 12,
        out_specs=vmem,
        scratch_shapes=[
            pltpu.SMEM(prefix_len.shape, jnp.int32),
            pltpu.SMEM(suffix_len.shape, jnp.int32),
            pltpu.VMEM((n,) + query_new.shape, bf),
            pltpu.VMEM(key_new.shape, bf),
            pltpu.VMEM(value_new.shape, bf),
            pltpu.VMEM(prefix_keys.shape, bf),
            pltpu.VMEM(prefix_values.shape, bf),
            pltpu.VMEM(sample_suffix_keys.shape[1:], bf),
            pltpu.VMEM(sample_suffix_values.shape[1:], bf),
            pltpu.VMEM(residual.shape, bf),
            pltpu.VMEM(out_weight.shape, bf),
            pltpu.VMEM(gain.shape, bf),
            pltpu.VMEM((rows, HEAD_SIZE), f32),
            pltpu.VMEM((rows, LANES), f32),
            pltpu.VMEM((rows, LANES), f32),
            pltpu.VMEM((rows, HEAD_SIZE), f32),
            pltpu.VMEM((rows, HEAD_SIZE), bf),
            pltpu.VMEM((n, rows // n, HEAD_SIZE), bf),
            pltpu.VMEM((n, 2, LANES), f32),
            pltpu.VMEM((n, 2, LANES), f32),
            pltpu.VMEM((n * frows, LANES), f32),
            pltpu.VMEM((n, frows, LANES), bf),
            pltpu.VMEM((n, frows, LANES), bf),
            dma((11,)),
            dma((CHUNKS,)),
            dma((n - 1,)),
            dma((n - 1,)),
            dma((n - 1,)),
            dma((n - 1,)),
            dma((n - 1,)),
            dma((n - 1,)),
            dma((CHUNKS * (n - 1),)),
            dma((CHUNKS * (n - 1),)),
        ],
        compiler_params=pltpu.CompilerParams(
            collective_id=0, has_side_effects=True, vmem_limit_bytes=62 * 1024 * 1024
        ),
    )(
        prefix_len,
        suffix_len,
        query_new,
        key_new,
        value_new,
        prefix_keys,
        prefix_values,
        sample_suffix_keys,
        sample_suffix_values,
        residual,
        out_weight,
        gain,
    )
    return (o[0:1], o[1:2])


def solution(mesh):
    placed = (
        P(("dp", "mp"), None),
        P(("dp", "mp"), None),
        P(("dp", "mp"), None),
        P(("dp", "mp"), None),
        P(("dp", "mp"), None),
        P(("dp", "mp"), None, None),
        P(("dp", "mp"), None, None),
        P("dp"),
        P(("dp", "mp")),
        P(("dp", "mp"), None),
        P("mp", None),
        P(),
    )
    return jax.shard_map(
        local,
        mesh=mesh,
        in_specs=placed,
        out_specs=(P(("dp", "mp"), None), P(("dp", "mp"), None)),
        check_vma=False,
    )
```

```python
import functools

import jax
import jax.numpy as jnp
from jax import lax
from jax.experimental import pallas as pl
from jax.experimental.pallas import tpu as pltpu
from jax.sharding import PartitionSpec as P

HEAD_SIZE = 128
KEY_VALUE_HEADS = 8
HQ = 32
GROUP = HQ // KEY_VALUE_HEADS
LANES = 128
LOW = -(2.0**100)
CHUNKS = 4
NT = (((1,), (1,)), ((), ()))


def head(ref, k):
    return ref[:, k * HEAD_SIZE : (k + 1) * HEAD_SIZE]


def kernel(
    n,
    plen_hbm,
    slen_hbm,
    q_hbm,
    kn_hbm,
    vn_hbm,
    pk_hbm,
    pv_hbm,
    sk_hbm,
    sv_hbm,
    res_hbm,
    w_hbm,
    gain_hbm,
    out_ref,
    plen_ref,
    slen_ref,
    qbuf,
    kn,
    vn,
    pk,
    pv,
    sk,
    sv,
    res,
    w,
    gain,
    q_rows,
    m0,
    l0,
    o0,
    pbuf,
    rbuf,
    tbuf,
    trecv,
    yacc,
    ysend,
    ybuf,
    local_sem,
    w_sem,
    q_send,
    q_recv,
    t_send,
    t_recv,
    p_send,
    p_recv,
    y_send,
    y_recv,
):
    me = lax.axis_index("mp")
    pre = pk.shape[0]
    suf = sk.shape[0]
    rows = pbuf.shape[0]
    part_rows = rows // n
    heads_dev = HQ // n
    width = w.shape[1]
    cw = width // CHUNKS
    crows = cw // LANES
    frows = width // LANES
    scale = HEAD_SIZE ** (-0.5)

    def peer(d):
        return lax.rem(me + d, n)

    upper = (me * 2) // n
    order = [(1 - upper) * (n - i) + upper * i for i in range(1, n)]

    local = [
        pltpu.make_async_copy(src, dst, local_sem.at[i])
        for i, (src, dst) in enumerate(
            (
                (q_hbm, qbuf.at[me]),
                (sk_hbm.at[0], sk),
                (kn_hbm, kn),
                (sv_hbm.at[0], sv),
                (vn_hbm, vn),
                (pk_hbm, pk),
                (pv_hbm, pv),
                (res_hbm, res),
                (gain_hbm, gain),
                (slen_hbm, slen_ref),
                (plen_hbm, plen_ref),
            )
        )
    ]
    for copy in local:
        copy.start()
    w_copies = [
        pltpu.make_async_copy(
            w_hbm.at[:, pl.ds(c * cw, cw)], w.at[:, pl.ds(c * cw, cw)], w_sem.at[c]
        )
        for c in range(CHUNKS)
    ]
    for copy in w_copies:
        copy.start()

    barrier = pltpu.get_barrier_semaphore()
    for d in range(1, n):
        pl.semaphore_signal(
            barrier, inc=1, device_id={"mp": peer(d)}, device_id_type=pl.DeviceIdType.MESH
        )
    pl.semaphore_wait(barrier, n - 1)

    local[0].wait()
    q_copies = []
    for d in order:
        copy = pltpu.make_async_remote_copy(
            src_ref=qbuf.at[me],
            dst_ref=qbuf.at[me],
            send_sem=q_send.at[d - 1],
            recv_sem=q_recv.at[d - 1],
            device_id={"mp": peer(d)},
            device_id_type=pl.DeviceIdType.MESH,
        )
        copy.start()
        q_copies.append(copy)

    m0[...] = jnp.full(m0.shape, LOW, jnp.float32)
    l0[...] = jnp.zeros(l0.shape, jnp.float32)
    o0[...] = jnp.zeros(o0.shape, jnp.float32)
    own = qbuf[me].astype(jnp.float32).reshape(HQ, HEAD_SIZE)
    own_bf = own.astype(jnp.bfloat16)
    head_of_row = lax.broadcasted_iota(jnp.int32, (HQ, 1), 0) // GROUP
    local[1].wait()
    local[2].wait()
    s_suf = jnp.zeros((HQ, suf), jnp.float32)
    key_rows = jnp.zeros((HQ, HEAD_SIZE), jnp.float32)
    for k in range(KEY_VALUE_HEADS):
        scores = lax.dot_general(own_bf, head(sk, k), NT, preferred_element_type=jnp.float32)
        s_suf = jnp.where(head_of_row == k, scores, s_suf)
        key_rows = jnp.where(head_of_row == k, head(kn, k).astype(jnp.float32), key_rows)
    s_new = jnp.sum(own * key_rows, axis=1, keepdims=True) * scale
    local[9].wait()
    svalid = lax.broadcasted_iota(jnp.int32, (HQ, suf), 1) < slen_ref[0]
    s_suf = jnp.where(svalid, s_suf * scale, LOW)
    top = jnp.maximum(jnp.max(s_suf, axis=1, keepdims=True), s_new)
    w_suf = jnp.where(svalid, jnp.exp(s_suf - top), 0.0)
    w_new = jnp.exp(s_new - top)
    own_total = jnp.sum(w_suf, axis=1, keepdims=True) + w_new
    w_bf = w_suf.astype(jnp.bfloat16)
    local[3].wait()
    local[4].wait()
    own_sum = jnp.zeros((HQ, HEAD_SIZE), jnp.float32)
    value_rows = jnp.zeros((HQ, HEAD_SIZE), jnp.float32)
    for k in range(KEY_VALUE_HEADS):
        sums = jnp.dot(w_bf, head(sv, k), preferred_element_type=jnp.float32)
        own_sum = jnp.where(head_of_row == k, sums, own_sum)
        value_rows = jnp.where(head_of_row == k, head(vn, k).astype(jnp.float32), value_rows)
    own_sum = own_sum + w_new.astype(jnp.bfloat16).astype(jnp.float32) * value_rows
    own_at = pl.ds(me, HQ, stride=n)
    m0[own_at, :] = jnp.broadcast_to(top, (HQ, LANES))
    l0[own_at, :] = jnp.broadcast_to(own_total, (HQ, LANES))
    o0[own_at, :] = own_sum

    local[5].wait()
    local[6].wait()
    for copy in q_copies:
        copy.wait_recv()
    for s in range(n):
        q_rows[pl.ds(s, HQ, stride=n), :] = qbuf[s].astype(jnp.float32).reshape(HQ, HEAD_SIZE)
    q_bf = q_rows[...].astype(jnp.bfloat16)
    per_kv = rows // KEY_VALUE_HEADS
    s_pre = jnp.concatenate(
        [
            lax.dot_general(
                q_bf[k * per_kv : (k + 1) * per_kv],
                head(pk, k),
                NT,
                preferred_element_type=jnp.float32,
            )
            for k in range(KEY_VALUE_HEADS)
        ],
        axis=0,
    )
    local[10].wait()
    pvalid = me * pre + lax.broadcasted_iota(jnp.int32, (rows, pre), 1) < plen_ref[0]
    s_pre = jnp.where(pvalid, s_pre * scale, LOW)
    top0 = m0[...]
    top = jnp.maximum(jnp.max(s_pre, axis=1, keepdims=True), top0)
    top = top.astype(jnp.bfloat16).astype(jnp.float32)
    w_pre = jnp.where(pvalid, jnp.exp(s_pre - top[:, :1]), 0.0)
    keep = jnp.exp(top0 - top)
    total = jnp.sum(w_pre, axis=1, keepdims=True) + l0[...] * keep
    w_bf = w_pre.astype(jnp.bfloat16)
    diagonal = lax.broadcasted_iota(jnp.int32, (part_rows, LANES), 0) == lax.broadcasted_iota(
        jnp.int32, (part_rows, LANES), 1
    )
    for s in range(n):
        at = slice(s * part_rows, (s + 1) * part_rows)
        for i, column in enumerate((top, total)):
            tbuf[s, i : i + 1, :] = jnp.sum(
                jnp.where(diagonal, column[at], 0.0), axis=0, keepdims=True
            )
    t_copies = []
    for d in order:
        copy = pltpu.make_async_remote_copy(
            src_ref=tbuf.at[peer(d)],
            dst_ref=trecv.at[me],
            send_sem=t_send.at[d - 1],
            recv_sem=t_recv.at[d - 1],
            device_id={"mp": peer(d)},
            device_id_type=pl.DeviceIdType.MESH,
        )
        t_copies.append(copy)
    sums = jnp.concatenate(
        [
            jnp.dot(
                w_bf[k * per_kv : (k + 1) * per_kv],
                head(pv, k),
                preferred_element_type=jnp.float32,
            )
            for k in range(KEY_VALUE_HEADS)
        ],
        axis=0,
    )
    sums = sums + o0[...] * keep
    pbuf[...] = sums.astype(jnp.bfloat16)
    for copy in t_copies:
        copy.start()

    p_copies = []
    for d in order:
        copy = pltpu.make_async_remote_copy(
            src_ref=pbuf.at[pl.ds(pl.multiple_of(peer(d) * part_rows, part_rows), part_rows)],
            dst_ref=rbuf.at[me],
            send_sem=p_send.at[d - 1],
            recv_sem=p_recv.at[d - 1],
            device_id={"mp": peer(d)},
            device_id_type=pl.DeviceIdType.MESH,
        )
        copy.start()
        p_copies.append(copy)
    rbuf[me] = pbuf[pl.ds(pl.multiple_of(me * part_rows, part_rows), part_rows), :]
    trecv[me] = tbuf[me]
    for copy in t_copies:
        copy.wait_recv()

    tops = [trecv[s, 0:1, :] for s in range(n)]
    best = functools.reduce(jnp.maximum, tops)
    factors = [jnp.exp(top_s - best) for top_s in tops]
    whole_total = sum(factors[s] * trecv[s, 1:2, :] for s in range(n))
    columns = [
        jnp.sum(jnp.where(diagonal, row, 0.0), axis=1, keepdims=True)
        for row in factors + [whole_total]
    ]
    for copy in p_copies:
        copy.wait_recv()
    whole_sum = sum(columns[s] * rbuf[s].astype(jnp.float32) for s in range(n))
    attn = whole_sum / columns[n]
    attn = jnp.concatenate([attn[h * n : (h + 1) * n] for h in range(heads_dev)], axis=1)
    attn = attn.astype(jnp.bfloat16)

    y_copies = []
    for c in range(CHUNKS):
        w_copies[c].wait()
        y = jnp.dot(attn, w[:, c * cw : (c + 1) * cw], preferred_element_type=jnp.float32)
        for j in range(crows):
            yacc[pl.ds(c * crows + j, n, stride=frows), :] = y[:, j * LANES : (j + 1) * LANES]
        at = pl.ds(c * crows, crows)
        for s in range(n):
            ysend[s, at, :] = yacc[pl.ds(s * frows + c * crows, crows), :].astype(jnp.bfloat16)
        for d in order:
            copy = pltpu.make_async_remote_copy(
                src_ref=ysend.at[peer(d), at],
                dst_ref=ybuf.at[me, at],
                send_sem=y_send.at[c * (n - 1) + d - 1],
                recv_sem=y_recv.at[c * (n - 1) + d - 1],
                device_id={"mp": peer(d)},
                device_id_type=pl.DeviceIdType.MESH,
            )
            copy.start()
            y_copies.append(copy)

    local[7].wait()
    local[8].wait()
    stream = res[...].astype(jnp.float32).reshape(frows, LANES)
    stream = stream + yacc[pl.ds(pl.multiple_of(me * frows, frows), frows), :]
    for copy in y_copies:
        copy.wait_recv()
    for d in range(1, n):
        stream = stream + ybuf[peer(d)].astype(jnp.float32)
    out_ref[0:1,:] = stream.astype(jnp.bfloat16).reshape(1,width)
    meansq = jnp.sum(stream * stream, keepdims=True) / width
    normed = stream * lax.rsqrt(meansq + 1e-05) * gain[...].astype(jnp.float32)
    out_ref[1:2,:] = normed.astype(jnp.bfloat16).reshape(1,width)
    for copy in q_copies + t_copies + p_copies + y_copies:
        copy.wait_send()


def local(
    query_new,
    key_new,
    value_new,
    prefix_keys,
    prefix_values,
    sample_suffix_keys,
    sample_suffix_values,
    prefix_len,
    suffix_len,
    residual,
    out_weight,
    norm_gain,
):
    n = lax.axis_size("mp")
    assert query_new.shape[0] == 1
    width = residual.shape[1]
    frows = width // LANES
    rows = HQ * n
    bf, f32 = jnp.bfloat16, jnp.float32
    gain = norm_gain.reshape(frows, LANES)
    hbm = pl.BlockSpec(memory_space=pltpu.HBM)
    vmem = pl.BlockSpec(memory_space=pltpu.VMEM)
    dma = pltpu.SemaphoreType.DMA
    o = pl.pallas_call(
        functools.partial(kernel, n),
        out_shape=pltpu.VMEM((2, width), bf),
        in_specs=[hbm] * 12,
        out_specs=vmem,
        scratch_shapes=[
            pltpu.SMEM(prefix_len.shape, jnp.int32),
            pltpu.SMEM(suffix_len.shape, jnp.int32),
            pltpu.VMEM((n,) + query_new.shape, bf),
            pltpu.VMEM(key_new.shape, bf),
            pltpu.VMEM(value_new.shape, bf),
            pltpu.VMEM(prefix_keys.shape, bf),
            pltpu.VMEM(prefix_values.shape, bf),
            pltpu.VMEM(sample_suffix_keys.shape[1:], bf),
            pltpu.VMEM(sample_suffix_values.shape[1:], bf),
            pltpu.VMEM(residual.shape, bf),
            pltpu.VMEM(out_weight.shape, bf),
            pltpu.VMEM(gain.shape, bf),
            pltpu.VMEM((rows, HEAD_SIZE), f32),
            pltpu.VMEM((rows, LANES), f32),
            pltpu.VMEM((rows, LANES), f32),
            pltpu.VMEM((rows, HEAD_SIZE), f32),
            pltpu.VMEM((rows, HEAD_SIZE), bf),
            pltpu.VMEM((n, rows // n, HEAD_SIZE), bf),
            pltpu.VMEM((n, 2, LANES), f32),
            pltpu.VMEM((n, 2, LANES), f32),
            pltpu.VMEM((n * frows, LANES), f32),
            pltpu.VMEM((n, frows, LANES), bf),
            pltpu.VMEM((n, frows, LANES), bf),
            dma((11,)),
            dma((CHUNKS,)),
            dma((n - 1,)),
            dma((n - 1,)),
            dma((n - 1,)),
            dma((n - 1,)),
            dma((n - 1,)),
            dma((n - 1,)),
            dma((CHUNKS * (n - 1),)),
            dma((CHUNKS * (n - 1),)),
        ],
        compiler_params=pltpu.CompilerParams(
            collective_id=0, has_side_effects=True, vmem_limit_bytes=62 * 1024 * 1024
        ),
    )(
        prefix_len,
        suffix_len,
        query_new,
        key_new,
        value_new,
        prefix_keys,
        prefix_values,
        sample_suffix_keys,
        sample_suffix_values,
        residual,
        out_weight,
        gain,
    )
    return (o[0:1], o[1:2])


def solution(mesh):
    placed = (
        P(("dp", "mp"), None),
        P(("dp", "mp"), None),
        P(("dp", "mp"), None),
        P(("dp", "mp"), None),
        P(("dp", "mp"), None),
        P(("dp", "mp"), None, None),
        P(("dp", "mp"), None, None),
        P("dp"),
        P(("dp", "mp")),
        P(("dp", "mp"), None),
        P("mp", None),
        P(),
    )
    return jax.shard_map(
        local,
        mesh=mesh,
        in_specs=placed,
        out_specs=(P(("dp", "mp"), None), P(("dp", "mp"), None)),
        check_vma=False,
    )
```
